256 devices in a mesh: gx: 4 (over y_lo, core), gz: 8 (over y_hi, x), ta: 8 (over z).
Axes of the slice: x: 4, y: 4 (y_hi: 2, y_lo: 2; y = y_hi * 2 + y_lo), z: 8, core: 2. Of those that a mesh axis runs over, the one named last changes fastest.
Arguments:
- links: float32 [4, 2, 3, 3, 32, 32, 512], P(None, None, None, None, 'ta', 'gz', 'gx'), may hold values from -1 to 1, as said below
Outputs:
- force: float32 [4, 2, 3, 3, 32, 32, 512], P(None, None, None, None, 'ta', 'gz', 'gx')
The draws below stay inside these ranges and needn't reach their ends.
Inputs may be any that keep to these rules, and one draw needn't show every extreme that they name: Every link matrix (real part links[mu, 0], imaginary part links[mu, 1]) is special unitary, up to float32 rounding.
All inputs are finite; a program needn't handle non-finite values.
Results may differ from the reference program's by a relative error of at most 0.0003.
Values sent between devices are 32-bit elements; how exact they have to be, the bound alone decides.
No kernel may reach another device: no remote copies, remote signals or barrier semaphores. Data moves between devices by JAX's collectives and lax.ppermute only.
A program may use at most 64 MiB of HBM per device.

```python
import jax
import jax.numpy as jnp

NX = 16
NY = 32
NZ = 32
NT = 32
NXY = 512


def draw_links(key, part):
    sample = jax.random.normal(key, (2, 4, 3, 3, NT, NZ, NXY), jnp.float32)
    real0 = sample[0][:, 0]
    imag0 = sample[1][:, 0]
    length0 = jnp.maximum(jnp.sqrt(jnp.sum(real0 * real0 + imag0 * imag0, axis=1, keepdims=True)), 1e-06)
    real0 = real0 / length0
    imag0 = imag0 / length0
    real1 = sample[0][:, 1]
    imag1 = sample[1][:, 1]
    inner_real = jnp.sum(real0 * real1 + imag0 * imag1, axis=1, keepdims=True)
    inner_imag = jnp.sum(real0 * imag1 - imag0 * real1, axis=1, keepdims=True)
    real1 = real1 - (inner_real * real0 - inner_imag * imag0)
    imag1 = imag1 - (inner_real * imag0 + inner_imag * real0)
    length1 = jnp.maximum(jnp.sqrt(jnp.sum(real1 * real1 + imag1 * imag1, axis=1, keepdims=True)), 1e-06)
    real1 = real1 / length1
    imag1 = imag1 / length1
    real_cols = []
    imag_cols = []
    for column in range(3):
        next_col = (column + 1) % 3
        last_col = (column + 2) % 3
        cross_real = real0[:, next_col] * real1[:, last_col] - imag0[:, next_col] * imag1[:, last_col] - real0[:, last_col] * real1[:, next_col] + imag0[:, last_col] * imag1[:, next_col]
        cross_imag = real0[:, next_col] * imag1[:, last_col] + imag0[:, next_col] * real1[:, last_col] - real0[:, last_col] * imag1[:, next_col] - imag0[:, last_col] * real1[:, next_col]
        real_cols.append(cross_real)
        imag_cols.append(-cross_imag)
    real2 = jnp.stack(real_cols, axis=1)
    imag2 = jnp.stack(imag_cols, axis=1)
    real_rows = jnp.stack([real0, real1, real2], axis=1)
    imag_rows = jnp.stack([imag0, imag1, imag2], axis=1)
    return jnp.stack([real_rows, imag_rows], axis=1)


def setup_inputs(seed: int = 0) -> dict:
    seeds = jax.random.split(jax.random.key(seed), 2)
    links = draw_links(jax.random.fold_in(seeds[1], 71), 0)
    return dict(links=links)


COEFF = -1.9


def matprod(left, right):
    total = left[:, 0][:, None] * right[0][None, :]
    total = total + left[:, 1][:, None] * right[1][None, :]
    return total + left[:, 2][:, None] * right[2][None, :]


def complex_mul(left, right):
    return (matprod(left[0], right[0]) - matprod(left[1], right[1]),
            matprod(left[0], right[1]) + matprod(left[1], right[0]))


def dagger(matrix):
    return (jnp.swapaxes(matrix[0], 0, 1), -jnp.swapaxes(matrix[1], 0, 1))


def unit_step(direction, sign):
    offset = [0, 0, 0, 0]
    offset[direction] = sign
    return tuple(offset)


def joined(first_step, second_step):
    return tuple(first_step[position] + second_step[position] for position in range(4))


def gauge_force(fetch_link):
    blocks = []
    still = (0, 0, 0, 0)
    for direction in range(4):
        ahead = unit_step(direction, 1)
        summed = None
        for transverse in range(4):
            if transverse == direction:
                continue
            side_up = unit_step(transverse, 1)
            side_down = unit_step(transverse, -1)
            upper = complex_mul(complex_mul(fetch_link(transverse, ahead), dagger(fetch_link(direction, side_up))),
                                dagger(fetch_link(transverse, still)))
            lower = complex_mul(complex_mul(dagger(fetch_link(transverse, joined(ahead, side_down))),
                                            dagger(fetch_link(direction, side_down))),
                                fetch_link(transverse, side_down))
            staple = (upper[0] + lower[0], upper[1] + lower[1])
            summed = staple if summed is None else (summed[0] + staple[0], summed[1] + staple[1])
        loop_matrix = complex_mul(fetch_link(direction, still), summed)
        real_part = 0.5 * (loop_matrix[0] - jnp.swapaxes(loop_matrix[0], 0, 1))
        imag_part = 0.5 * (loop_matrix[1] + jnp.swapaxes(loop_matrix[1], 0, 1))
        trace_third = (loop_matrix[1][0, 0] + loop_matrix[1][1, 1] + loop_matrix[1][2, 2]) / 3.0
        identity = jnp.eye(3, dtype=jnp.float32).reshape((3, 3) + (1,) * trace_third.ndim)
        imag_part = imag_part - identity * trace_third
        blocks.append(COEFF * jnp.stack([real_part, imag_part], axis=0))
    return jnp.stack(blocks, axis=0)


def reference(links):
    lattice = links.reshape(links.shape[:6] + (NY, NX))

    def fetch_link(direction, offset):
        field = lattice[direction]
        field = jnp.roll(field, (-offset[0], -offset[1], -offset[2], -offset[3]), axis=(3, 4, 5, 6))
        return (field[0], field[1])

    return gauge_force(fetch_link).reshape(links.shape)
```

```python
import jax
import jax.numpy as jnp
from jax import lax
from jax.experimental import pallas as pl
from jax.experimental.pallas import tpu as pltpu
from jax.sharding import PartitionSpec as P

NX = 16
COEFF = -1.9

ROWS = 16
LANES = 128
TIMES = 4
DEPTHS = 4
PAIRS = ((0, 1), (0, 2), (0, 3), (1, 2), (1, 3), (2, 3))
OTHERS = tuple(tuple(d for d in range(4) if d != face) for face in range(3))


def comp(direction, part, row, col):
    return ((direction * 2 + part) * 3 + row) * 3 + col


def face_comp(slot, part, row, col):
    return ((slot * 2 + part) * 2 + row) * 3 + col


def accumulate(terms):
    total = None
    for sign, left, right in terms:
        product = left * right
        if total is None:
            total = product if sign > 0 else -product
        else:
            total = total + product if sign > 0 else total - product
    return total


def product_rows(left, right):
    out = []
    for row in left:
        cols = []
        for j in range(3):
            re = accumulate(
                [(1, row[k][0], right[k][j][0]) for k in range(3)]
                + [(-1, row[k][1], right[k][j][1]) for k in range(3)]
            )
            im = accumulate(
                [(1, row[k][0], right[k][j][1]) for k in range(3)]
                + [(1, row[k][1], right[k][j][0]) for k in range(3)]
            )
            cols.append((re, im))
        out.append(cols)
    return out


def product_rows_dagger(left, right):
    out = []
    for row in left:
        cols = []
        for j in range(3):
            re = accumulate(
                [(1, row[k][0], right[j][k][0]) for k in range(3)]
                + [(1, row[k][1], right[j][k][1]) for k in range(3)]
            )
            im = accumulate(
                [(1, row[k][1], right[j][k][0]) for k in range(3)]
                + [(-1, row[k][0], right[j][k][1]) for k in range(3)]
            )
            cols.append((re, im))
        out.append(cols)
    return out


def cross_real(row0, row1, j):
    a, b = (j + 1) % 3, (j + 2) % 3
    return accumulate(
        [
            (1, row0[a][0], row1[b][0]),
            (-1, row0[a][1], row1[b][1]),
            (-1, row0[b][0], row1[a][0]),
            (1, row0[b][1], row1[a][1]),
        ]
    )


def cross_imag(row0, row1, j):
    a, b = (j + 1) % 3, (j + 2) % 3
    return accumulate(
        [
            (1, row0[b][0], row1[a][1]),
            (1, row0[b][1], row1[a][0]),
            (-1, row0[a][0], row1[b][1]),
            (-1, row0[a][1], row1[b][0]),
        ]
    )


def third_row(row0, row1):
    return [(cross_real(row0, row1, j), cross_imag(row0, row1, j)) for j in range(3)]


def plaquette(left, left_ahead, right, right_ahead):
    first = product_rows(left[:2], left_ahead)
    second = product_rows(right[:2], right_ahead)
    second.append(third_row(second[0], second[1]))
    loop = product_rows_dagger(first, second)
    row0, row1 = loop
    re20 = cross_real(row0, row1, 0)
    im20 = cross_imag(row0, row1, 0)
    re21 = cross_real(row0, row1, 1)
    im21 = cross_imag(row0, row1, 1)
    im22 = cross_imag(row0, row1, 2)
    third = (row0[0][1] + row1[1][1] + im22) * (1.0 / 3.0)
    d0 = row0[0][1] - third
    d1 = row1[1][1] - third
    return [
        row0[1][0] - row1[0][0],
        row0[1][1] + row1[0][1],
        row0[2][0] - re20,
        row0[2][1] + im20,
        row1[2][0] - re21,
        row1[2][1] + im21,
        d0 + d0,
        d1 + d1,
    ]


def rotated(force, link):
    r01, i01, r02, i02, r12, i12, d0, d1 = force
    d2 = -(d0 + d1)
    diag = (d0, d1, d2)
    upper = {(0, 1): (r01, i01), (0, 2): (r02, i02), (1, 2): (r12, i12)}
    columns = []
    for j in range(3):
        entries = []
        for k in range(3):
            re_terms = [(-1, diag[k], link[k][j][1])]
            im_terms = [(1, diag[k], link[k][j][0])]
            for l in range(3):
                if l == k:
                    continue
                if l > k:
                    re, im = upper[(k, l)]
                    sign = 1
                else:
                    re, im = upper[(l, k)]
                    sign = -1
                re_terms = [(sign, re, link[l][j][0])] + re_terms + [(-1, im, link[l][j][1])]
                im_terms = [(1, im, link[l][j][0])] + im_terms + [(sign, re, link[l][j][1])]
            re_terms.sort(key=lambda term: -term[0])
            entries.append((accumulate(re_terms), accumulate(im_terms)))
        columns.append(entries)

    def real(i, j):
        return accumulate(
            [(1, link[k][i][0], columns[j][k][0]) for k in range(3)]
            + [(1, link[k][i][1], columns[j][k][1]) for k in range(3)]
        )

    def imag(i, j):
        return accumulate(
            [(1, link[k][i][0], columns[j][k][1]) for k in range(3)]
            + [(-1, link[k][i][1], columns[j][k][0]) for k in range(3)]
        )

    return [real(0, 1), imag(0, 1), real(0, 2), imag(0, 2), real(1, 2), imag(1, 2), imag(0, 0), imag(1, 1)]


def lane_group(shape):
    return lax.broadcasted_iota(jnp.int32, shape, 1) // NX


def row_index(shape):
    return lax.broadcasted_iota(jnp.int32, shape, 0)


def turned(value, groups):
    return pltpu.roll(value, groups % 8 * NX, 1) if groups % 8 else value


def packed(values, last):
    total = None
    for group, value in enumerate(values):
        value = turned(value, group + 1 if last else group)
        total = value if total is None else jnp.where(lane_group(value.shape) == group, value, total)
    return total


def unpacked(value, group, last):
    return turned(value, 7 - group if last else -group)


def send_kernel(links, time_out, depth_out, plane_out):
    for face, out in ((0, time_out), (1, depth_out)):
        for slot, direction in enumerate(OTHERS[face]):
            for part in range(2):
                for row in range(2):
                    for col in range(3):
                        source = comp(direction, part, row, col)
                        target = face_comp(slot, part, row, col) * 4
                        if face == 0:
                            out[target : target + 4] = links[source, 0:DEPTHS]
                        else:
                            out[target : target + 4] = links[source, pl.ds(0, TIMES, stride=DEPTHS)]
    for part in range(2):
        for row in range(2):
            for col in range(3):
                target = ((part * 2 + row) * 3 + col) * 8
                plane_out[target : target + 8] = packed(
                    [
                        links[comp(direction, part, row, col), 8 * half : 8 * half + 8]
                        for half in range(2)
                        for direction in OTHERS[2]
                    ],
                    False,
                )


def matrix(ref, base, rows):
    return [
        [(ref[base + row * 3 + col, rows], ref[base + 9 + row * 3 + col, rows]) for col in range(3)]
        for row in range(3)
    ]


def face_matrix(ref, slot, size):
    rows = [
        [
            tuple(
                ref[face_comp(slot, part, row, col) * size : (face_comp(slot, part, row, col) + 1) * size]
                for part in range(2)
            )
            for col in range(3)
        ]
        for row in range(2)
    ]
    rows.append(third_row(rows[0], rows[1]))
    return rows


def shift_links(links, time_in, depth_in, plane_in, shifted):
    column = lax.broadcasted_iota(jnp.int32, (8, LANES), 1) % NX
    right_edge = column == NX - 1
    last_plane = lane_group((8, LANES)) == LANES // NX - 1
    for face in range(2):
        received = time_in if face == 0 else depth_in
        for slot, direction in enumerate(OTHERS[face]):
            halo = face_matrix(received, slot, 4)
            for part in range(2):
                for row in range(3):
                    for col in range(3):
                        c = comp(direction, part, row, col)
                        if face == 0:
                            shifted[0, c, 0 : ROWS - 4] = links[c, 4:ROWS]
                            shifted[0, c, ROWS - 4 : ROWS] = halo[row][col][part]
                        else:
                            shifted[1, c, 0 : ROWS - 1] = links[c, 1:ROWS]
                            shifted[1, c, pl.ds(3, TIMES, stride=DEPTHS)] = halo[row][col][part]
    halo = face_matrix(plane_in, 0, 8)
    for part in range(2):
        for row in range(3):
            for col in range(3):
                for slot, direction in enumerate(OTHERS[2]):
                    c = comp(direction, part, row, col)
                    for half in range(2):
                        rows = slice(8 * half, 8 * half + 8)
                        outer = unpacked(halo[row][col][part], 3 * half + slot, True)
                        shifted[2, c, rows] = jnp.where(last_plane, outer, turned(links[c, rows], 7))
    for direction in range(3):
        for offset in range(18):
            c = direction * 18 + offset
            for half in range(2):
                rows = slice(8 * half, 8 * half + 8)
                value = links[c, rows]
                shifted[3, c, rows] = jnp.where(
                    right_edge, pltpu.roll(value, NX - 1, 1), pltpu.roll(value, LANES - 1, 1)
                )


def main_kernel(
    links, time_in, depth_in, plane_in, force, time_out, depth_out, plane_out, shifted, moved, plane
):
    shift_links(links, time_in, depth_in, plane_in, shifted)
    for face in range(2):
        for c in range(24):
            moved[face, c, 0:8] = jnp.zeros((8, LANES), jnp.float32)

    def step(half, carry):
        start = pl.multiple_of(half * 8, 8)
        rows = pl.ds(start, 8)
        column = lax.broadcasted_iota(jnp.int32, (8, LANES), 1)
        left_edge = column % NX == 0
        first_plane = column < NX
        fresh = [True] * 4

        def add(direction, values, sign):
            for i in range(8):
                c = direction * 8 + i
                if fresh[direction]:
                    force[c, rows] = values[i] if sign > 0 else -values[i]
                elif sign > 0:
                    force[c, rows] = force[c, rows] + values[i]
                else:
                    force[c, rows] = force[c, rows] - values[i]
            fresh[direction] = False

        def carry_over(direction, step_direction, values, sign):
            if step_direction < 2:
                slot = OTHERS[step_direction].index(direction)
                lower = pl.ds(pl.multiple_of(start + 8, 8), 8)
                for i in range(8):
                    moved[step_direction, slot * 8 + i, lower] = values[i] if sign > 0 else -values[i]
                return
            if step_direction == 2:
                slot = OTHERS[2].index(direction)
                for i in range(8):
                    plane[slot * 8 + i, rows] = values[i] if sign > 0 else -values[i]
                values = [jnp.where(first_plane, 0.0, turned(v, 1)) for v in values]
            else:
                values = [
                    jnp.where(left_edge, pltpu.roll(v, LANES - NX + 1, 1), pltpu.roll(v, 1, 1))
                    for v in values
                ]
            add(direction, values, sign)

        for mu, nu in PAIRS:
            link_mu = matrix(links, mu * 18, rows)
            link_nu = matrix(links, nu * 18, rows)
            values = plaquette(
                link_mu,
                matrix(shifted.at[mu], nu * 18, rows),
                link_nu,
                matrix(shifted.at[nu], mu * 18, rows),
            )
            add(mu, values, 1)
            add(nu, values, -1)
            carry_over(mu, nu, rotated(values, link_nu), -1)
            carry_over(nu, mu, rotated(values, link_mu), 1)
        return carry

    lax.fori_loop(0, 2, step, 0)

    inner = row_index((8, LANES)) % DEPTHS != 0
    for direction in range(4):
        for i in range(8):
            c = direction * 8 + i
            for half in range(2):
                rows = slice(8 * half, 8 * half + 8)
                total = force[c, rows]
                if direction != 0:
                    slot = OTHERS[0].index(direction) * 8 + i
                    total = total + moved[0, slot, 8 * half + 4 : 8 * half + 12]
                if direction != 1:
                    slot = OTHERS[1].index(direction) * 8 + i
                    total = total + jnp.where(inner, moved[1, slot, 8 * half + 7 : 8 * half + 15], 0.0)
                force[c, rows] = total
    for c in range(24):
        time_out[4 * c : 4 * c + 4] = moved[0, c, 20:24]
        depth_out[4 * c : 4 * c + 4] = moved[1, c, pl.ds(11, TIMES, stride=DEPTHS)]
    for i in range(8):
        plane_out[8 * i : 8 * i + 8] = packed(
            [plane[slot * 8 + i, 8 * half : 8 * half + 8] for half in range(2) for slot in range(3)], True
        )


def final_kernel(force, time_in, depth_in, plane_in, out, work):
    first_plane = lax.broadcasted_iota(jnp.int32, (8, LANES), 1) < NX
    for direction in range(4):
        for i in range(8):
            c = direction * 8 + i
            for half in range(2):
                rows = slice(8 * half, 8 * half + 8)
                total = force[c, rows]
                if direction != 2:
                    group = 3 * half + OTHERS[2].index(direction)
                    outer = unpacked(plane_in[8 * i : 8 * i + 8], group, False)
                    total = total + jnp.where(first_plane, outer, 0.0)
                work[c, rows] = total
            if direction != 0:
                at = (OTHERS[0].index(direction) * 8 + i) * 4
                work[c, 0:4] = work[c, 0:4] + time_in[at : at + 4]
            if direction != 1:
                at = (OTHERS[1].index(direction) * 8 + i) * 4
                sites = pl.ds(0, TIMES, stride=DEPTHS)
                work[c, sites] = work[c, sites] + depth_in[at : at + 4]
        half_coeff = 0.5 * COEFF
        upper = ((0, 1), (0, 2), (1, 2))
        for half in range(2):
            rows = slice(8 * half, 8 * half + 8)
            for n, (row, col) in enumerate(upper):
                re = work[direction * 8 + 2 * n, rows] * half_coeff
                im = work[direction * 8 + 2 * n + 1, rows] * half_coeff
                out[comp(direction, 0, row, col), rows] = re
                out[comp(direction, 0, col, row), rows] = -re
                out[comp(direction, 1, row, col), rows] = im
                out[comp(direction, 1, col, row), rows] = im
            d0 = work[direction * 8 + 6, rows] * half_coeff
            d1 = work[direction * 8 + 7, rows] * half_coeff
            zero = jnp.zeros_like(d0)
            for k, value in enumerate((d0, d1, -(d0 + d1))):
                out[comp(direction, 1, k, k), rows] = value
                out[comp(direction, 0, k, k), rows] = zero


def shape(*dims):
    return jax.ShapeDtypeStruct(dims, jnp.float32)


def move(value, axis, forward):
    count = lax.axis_size(axis)
    step = 1 if forward else count - 1
    return lax.ppermute(value, axis, [(i, (i + step) % count) for i in range(count)])


def per_device(links):
    flat = links.reshape(72, ROWS, LANES)
    faces = pl.pallas_call(
        send_kernel, out_shape=(shape(144, LANES), shape(144, LANES), shape(96, LANES)), name="send"
    )(flat)
    depth = move(faces[1], "gz", False)
    time = move(faces[0], "ta", False)
    plane = move(faces[2], "gx", False)
    force, time, depth, plane = pl.pallas_call(
        main_kernel,
        out_shape=(shape(32, ROWS, LANES), shape(96, LANES), shape(96, LANES), shape(64, LANES)),
        scratch_shapes=[
            pltpu.VMEM((4, 72, ROWS, LANES), jnp.float32),
            pltpu.VMEM((2, 24, 24, LANES), jnp.float32),
            pltpu.VMEM((24, ROWS, LANES), jnp.float32),
        ],
        name="main",
    )(flat, time, depth, plane)
    depth = move(depth, "gz", True)
    time = move(time, "ta", True)
    plane = move(plane, "gx", True)
    out = pl.pallas_call(
        final_kernel,
        out_shape=shape(72, ROWS, LANES),
        scratch_shapes=[pltpu.VMEM((32, ROWS, LANES), jnp.float32)],
        name="final",
    )(force, time, depth, plane)
    return out.reshape(links.shape)


def solution(mesh):
    spec = P(None, None, None, None, "ta", "gz", "gx")
    return jax.shard_map(per_device, mesh=mesh, in_specs=(spec,), out_specs=spec, check_vma=False)
```

```python
import jax
import jax.numpy as jnp
from jax import lax
from jax.experimental import pallas as pl
from jax.experimental.pallas import tpu as pltpu
from jax.sharding import PartitionSpec as P

NX = 16
COEFF = -1.9

ROWS = 16
LANES = 128
TIMES = 4
DEPTHS = 4
PAIRS = ((0, 1), (0, 2), (0, 3), (1, 2), (1, 3), (2, 3))
OTHERS = tuple(tuple(d for d in range(4) if d != face) for face in range(3))


def comp(direction, part, row, col):
    return ((direction * 2 + part) * 3 + row) * 3 + col


def face_comp(slot, part, row, col):
    return ((slot * 2 + part) * 2 + row) * 3 + col


def accumulate(terms):
    total = None
    for sign, left, right in terms:
        product = left * right
        if total is None:
            total = product if sign > 0 else -product
        else:
            total = total + product if sign > 0 else total - product
    return total


def product_rows(left, right):
    out = []
    for row in left:
        cols = []
        for j in range(3):
            re = accumulate(
                [(1, row[k][0], right[k][j][0]) for k in range(3)]
                + [(-1, row[k][1], right[k][j][1]) for k in range(3)]
            )
            im = accumulate(
                [(1, row[k][0], right[k][j][1]) for k in range(3)]
                + [(1, row[k][1], right[k][j][0]) for k in range(3)]
            )
            cols.append((re, im))
        out.append(cols)
    return out


def product_rows_dagger(left, right):
    out = []
    for row in left:
        cols = []
        for j in range(3):
            re = accumulate(
                [(1, row[k][0], right[j][k][0]) for k in range(3)]
                + [(1, row[k][1], right[j][k][1]) for k in range(3)]
            )
            im = accumulate(
                [(1, row[k][1], right[j][k][0]) for k in range(3)]
                + [(-1, row[k][0], right[j][k][1]) for k in range(3)]
            )
            cols.append((re, im))
        out.append(cols)
    return out


def cross_real(row0, row1, j):
    a, b = (j + 1) % 3, (j + 2) % 3
    return accumulate(
        [
            (1, row0[a][0], row1[b][0]),
            (-1, row0[a][1], row1[b][1]),
            (-1, row0[b][0], row1[a][0]),
            (1, row0[b][1], row1[a][1]),
        ]
    )


def cross_imag(row0, row1, j):
    a, b = (j + 1) % 3, (j + 2) % 3
    return accumulate(
        [
            (1, row0[b][0], row1[a][1]),
            (1, row0[b][1], row1[a][0]),
            (-1, row0[a][0], row1[b][1]),
            (-1, row0[a][1], row1[b][0]),
        ]
    )


def third_row(row0, row1):
    return [(cross_real(row0, row1, j), cross_imag(row0, row1, j)) for j in range(3)]


def plaquette(left, left_ahead, right, right_ahead):
    first = product_rows(left[:2], left_ahead)
    second = product_rows(right[:2], right_ahead)
    second.append(third_row(second[0], second[1]))
    loop = product_rows_dagger(first, second)
    row0, row1 = loop
    re20 = cross_real(row0, row1, 0)
    im20 = cross_imag(row0, row1, 0)
    re21 = cross_real(row0, row1, 1)
    im21 = cross_imag(row0, row1, 1)
    im22 = cross_imag(row0, row1, 2)
    third = (row0[0][1] + row1[1][1] + im22) * (1.0 / 3.0)
    d0 = row0[0][1] - third
    d1 = row1[1][1] - third
    return [
        row0[1][0] - row1[0][0],
        row0[1][1] + row1[0][1],
        row0[2][0] - re20,
        row0[2][1] + im20,
        row1[2][0] - re21,
        row1[2][1] + im21,
        d0 + d0,
        d1 + d1,
    ]


def rotated(force, link):
    r01, i01, r02, i02, r12, i12, d0, d1 = force
    d2 = -(d0 + d1)
    diag = (d0, d1, d2)
    upper = {(0, 1): (r01, i01), (0, 2): (r02, i02), (1, 2): (r12, i12)}
    columns = []
    for j in range(3):
        entries = []
        for k in range(3):
            re_terms = [(-1, diag[k], link[k][j][1])]
            im_terms = [(1, diag[k], link[k][j][0])]
            for l in range(3):
                if l == k:
                    continue
                if l > k:
                    re, im = upper[(k, l)]
                    sign = 1
                else:
                    re, im = upper[(l, k)]
                    sign = -1
                re_terms = [(sign, re, link[l][j][0])] + re_terms + [(-1, im, link[l][j][1])]
                im_terms = [(1, im, link[l][j][0])] + im_terms + [(sign, re, link[l][j][1])]
            re_terms.sort(key=lambda term: -term[0])
            entries.append((accumulate(re_terms), accumulate(im_terms)))
        columns.append(entries)

    def real(i, j):
        return accumulate(
            [(1, link[k][i][0], columns[j][k][0]) for k in range(3)]
            + [(1, link[k][i][1], columns[j][k][1]) for k in range(3)]
        )

    def imag(i, j):
        return accumulate(
            [(1, link[k][i][0], columns[j][k][1]) for k in range(3)]
            + [(-1, link[k][i][1], columns[j][k][0]) for k in range(3)]
        )

    return [real(0, 1), imag(0, 1), real(0, 2), imag(0, 2), real(1, 2), imag(1, 2), imag(0, 0), imag(1, 1)]


def lane_group(shape):
    return lax.broadcasted_iota(jnp.int32, shape, 1) // NX


def row_index(shape):
    return lax.broadcasted_iota(jnp.int32, shape, 0)


def turned(value, groups):
    return pltpu.roll(value, groups % 8 * NX, 1) if groups % 8 else value


def packed(values, last):
    total = None
    for group, value in enumerate(values):
        value = turned(value, group + 1 if last else group)
        total = value if total is None else jnp.where(lane_group(value.shape) == group, value, total)
    return total


def unpacked(value, group, last):
    return turned(value, 7 - group if last else -group)


def send_kernel(links, time_out, depth_out, plane_out):
    for face, out in ((0, time_out), (1, depth_out)):
        for slot, direction in enumerate(OTHERS[face]):
            for part in range(2):
                for row in range(2):
                    for col in range(3):
                        source = comp(direction, part, row, col)
                        target = face_comp(slot, part, row, col) * 4
                        if face == 0:
                            out[target : target + 4] = links[source, 0:DEPTHS]
                        else:
                            out[target : target + 4] = links[source, pl.ds(0, TIMES, stride=DEPTHS)]
    for part in range(2):
        for row in range(2):
            for col in range(3):
                target = ((part * 2 + row) * 3 + col) * 8
                plane_out[target : target + 8] = packed(
                    [
                        links[comp(direction, part, row, col), 8 * half : 8 * half + 8]
                        for half in range(2)
                        for direction in OTHERS[2]
                    ],
                    False,
                )


def matrix(ref, base, rows):
    return [
        [(ref[base + row * 3 + col, rows], ref[base + 9 + row * 3 + col, rows]) for col in range(3)]
        for row in range(3)
    ]


def face_matrix(ref, slot, size):
    rows = [
        [
            tuple(
                ref[face_comp(slot, part, row, col) * size : (face_comp(slot, part, row, col) + 1) * size]
                for part in range(2)
            )
            for col in range(3)
        ]
        for row in range(2)
    ]
    rows.append(third_row(rows[0], rows[1]))
    return rows


def shift_links(links, time_in, depth_in, plane_in, shifted):
    column = lax.broadcasted_iota(jnp.int32, (8, LANES), 1) % NX
    right_edge = column == NX - 1
    last_plane = lane_group((8, LANES)) == LANES // NX - 1
    for face in range(2):
        received = time_in if face == 0 else depth_in
        for slot, direction in enumerate(OTHERS[face]):
            halo = face_matrix(received, slot, 4)
            for part in range(2):
                for row in range(3):
                    for col in range(3):
                        c = comp(direction, part, row, col)
                        if face == 0:
                            shifted[0, c, 0 : ROWS - 4] = links[c, 4:ROWS]
                            shifted[0, c, ROWS - 4 : ROWS] = halo[row][col][part]
                        else:
                            shifted[1, c, 0 : ROWS - 1] = links[c, 1:ROWS]
                            shifted[1, c, pl.ds(3, TIMES, stride=DEPTHS)] = halo[row][col][part]
    halo = face_matrix(plane_in, 0, 8)
    for part in range(2):
        for row in range(3):
            for col in range(3):
                for slot, direction in enumerate(OTHERS[2]):
                    c = comp(direction, part, row, col)
                    for half in range(2):
                        rows = slice(8 * half, 8 * half + 8)
                        outer = unpacked(halo[row][col][part], 3 * half + slot, True)
                        shifted[2, c, rows] = jnp.where(last_plane, outer, turned(links[c, rows], 7))
    for direction in range(3):
        for offset in range(18):
            c = direction * 18 + offset
            for half in range(2):
                rows = slice(8 * half, 8 * half + 8)
                value = links[c, rows]
                shifted[3, c, rows] = jnp.where(
                    right_edge, pltpu.roll(value, NX - 1, 1), pltpu.roll(value, LANES - 1, 1)
                )


def main_kernel(
    links, time_in, depth_in, plane_in, force, time_out, depth_out, plane_out, shifted, moved, plane
):
    shift_links(links, time_in, depth_in, plane_in, shifted)
    for face in range(2):
        for c in range(24):
            moved[face, c, 0:8] = jnp.zeros((8, LANES), jnp.float32)

    def step(half, carry):
        start = pl.multiple_of(half * 8, 8)
        rows = pl.ds(start, 8)
        column = lax.broadcasted_iota(jnp.int32, (8, LANES), 1)
        left_edge = column % NX == 0
        first_plane = column < NX
        fresh = [True] * 4

        def add(direction, values, sign):
            for i in range(8):
                c = direction * 8 + i
                if fresh[direction]:
                    force[c, rows] = values[i] if sign > 0 else -values[i]
                elif sign > 0:
                    force[c, rows] = force[c, rows] + values[i]
                else:
                    force[c, rows] = force[c, rows] - values[i]
            fresh[direction] = False

        def carry_over(direction, step_direction, values, sign):
            if step_direction < 2:
                slot = OTHERS[step_direction].index(direction)
                lower = pl.ds(pl.multiple_of(start + 8, 8), 8)
                for i in range(8):
                    moved[step_direction, slot * 8 + i, lower] = values[i] if sign > 0 else -values[i]
                return
            if step_direction == 2:
                slot = OTHERS[2].index(direction)
                for i in range(8):
                    plane[slot * 8 + i, rows] = values[i] if sign > 0 else -values[i]
                values = [jnp.where(first_plane, 0.0, turned(v, 1)) for v in values]
            else:
                values = [
                    jnp.where(left_edge, pltpu.roll(v, LANES - NX + 1, 1), pltpu.roll(v, 1, 1))
                    for v in values
                ]
            add(direction, values, sign)

        for mu, nu in PAIRS:
            link_mu = matrix(links, mu * 18, rows)
            link_nu = matrix(links, nu * 18, rows)
            values = plaquette(
                link_mu,
                matrix(shifted.at[mu], nu * 18, rows),
                link_nu,
                matrix(shifted.at[nu], mu * 18, rows),
            )
            add(mu, values, 1)
            add(nu, values, -1)
            carry_over(mu, nu, rotated(values, link_nu), -1)
            carry_over(nu, mu, rotated(values, link_mu), 1)
        return carry

    lax.fori_loop(0, 2, step, 0)

    inner = row_index((8, LANES)) % DEPTHS != 0
    for direction in range(4):
        for i in range(8):
            c = direction * 8 + i
            for half in range(2):
                rows = slice(8 * half, 8 * half + 8)
                total = force[c, rows]
                if direction != 0:
                    slot = OTHERS[0].index(direction) * 8 + i
                    total = total + moved[0, slot, 8 * half + 4 : 8 * half + 12]
                if direction != 1:
                    slot = OTHERS[1].index(direction) * 8 + i
                    total = total + jnp.where(inner, moved[1, slot, 8 * half + 7 : 8 * half + 15], 0.0)
                force[c, rows] = total
    for c in range(24):
        time_out[4 * c : 4 * c + 4] = moved[0, c, 20:24]
        depth_out[4 * c : 4 * c + 4] = moved[1, c, pl.ds(11, TIMES, stride=DEPTHS)]
    for i in range(8):
        plane_out[8 * i : 8 * i + 8] = packed(
            [plane[slot * 8 + i, 8 * half : 8 * half + 8] for half in range(2) for slot in range(3)], True
        )


def final_kernel(force, time_in, depth_in, plane_in, out, work):
    first_plane = lax.broadcasted_iota(jnp.int32, (8, LANES), 1) < NX
    for direction in range(4):
        for i in range(8):
            c = direction * 8 + i
            for half in range(2):
                rows = slice(8 * half, 8 * half + 8)
                total = force[c, rows]
                if direction != 2:
                    group = 3 * half + OTHERS[2].index(direction)
                    outer = unpacked(plane_in[8 * i : 8 * i + 8], group, False)
                    total = total + jnp.where(first_plane, outer, 0.0)
                work[c, rows] = total
            if direction != 0:
                at = (OTHERS[0].index(direction) * 8 + i) * 4
                work[c, 0:4] = work[c, 0:4] + time_in[at : at + 4]
            if direction != 1:
                at = (OTHERS[1].index(direction) * 8 + i) * 4
                sites = pl.ds(0, TIMES, stride=DEPTHS)
                work[c, sites] = work[c, sites] + depth_in[at : at + 4]
        half_coeff = 0.5 * COEFF
        upper = ((0, 1), (0, 2), (1, 2))
        for half in range(2):
            rows = slice(8 * half, 8 * half + 8)
            for n, (row, col) in enumerate(upper):
                re = work[direction * 8 + 2 * n, rows] * half_coeff
                im = work[direction * 8 + 2 * n + 1, rows] * half_coeff
                out[comp(direction, 0, row, col), rows] = re
                out[comp(direction, 0, col, row), rows] = -re
                out[comp(direction, 1, row, col), rows] = im
                out[comp(direction, 1, col, row), rows] = im
            d0 = work[direction * 8 + 6, rows] * half_coeff
            d1 = work[direction * 8 + 7, rows] * half_coeff
            zero = jnp.zeros_like(d0)
            for k, value in enumerate((d0, d1, -(d0 + d1))):
                out[comp(direction, 1, k, k), rows] = value
                out[comp(direction, 0, k, k), rows] = zero


def shape(*dims):
    return pltpu.VMEM(dims, jnp.float32)


def move(value, axis, forward):
    count = lax.axis_size(axis)
    step = 1 if forward else count - 1
    moved = lax.ppermute(value, axis, [(i, (i + step) % count) for i in range(count)])
    return pltpu.with_memory_space_constraint(moved, pltpu.VMEM)


def per_device(links):
    flat = pltpu.with_memory_space_constraint(links.reshape(72, ROWS, LANES), pltpu.VMEM)
    faces = pl.pallas_call(
        send_kernel, out_shape=(shape(144, LANES), shape(144, LANES), shape(96, LANES)), name="send"
    )(flat)
    depth = move(faces[1], "gz", False)
    time = move(faces[0], "ta", False)
    plane = move(faces[2], "gx", False)
    force, time, depth, plane = pl.pallas_call(
        main_kernel,
        out_shape=(shape(32, ROWS, LANES), shape(96, LANES), shape(96, LANES), shape(64, LANES)),
        scratch_shapes=[
            pltpu.VMEM((4, 72, ROWS, LANES), jnp.float32),
            pltpu.VMEM((2, 24, 24, LANES), jnp.float32),
            pltpu.VMEM((24, ROWS, LANES), jnp.float32),
        ],
        name="main",
    )(flat, time, depth, plane)
    depth = move(depth, "gz", True)
    time = move(time, "ta", True)
    plane = move(plane, "gx", True)
    out = pl.pallas_call(
        final_kernel,
        out_shape=jax.ShapeDtypeStruct((72, ROWS, LANES), jnp.float32),
        scratch_shapes=[pltpu.VMEM((32, ROWS, LANES), jnp.float32)],
        name="final",
    )(pltpu.with_memory_space_constraint(force, pltpu.VMEM), time, depth, plane)
    return out.reshape(links.shape)


def solution(mesh):
    spec = P(None, None, None, None, "ta", "gz", "gx")
    return jax.shard_map(per_device, mesh=mesh, in_specs=(spec,), out_specs=spec, check_vma=False)
```

```python
import jax
import jax.numpy as jnp
from jax import lax
from jax.experimental import pallas as pl
from jax.experimental.pallas import tpu as pltpu
from jax.sharding import PartitionSpec as P


NX = 16
COEFF = -1.9

ROWS = 16
LANES = 128
TIMES = 4
DEPTHS = 4
PAIRS = ((0, 1), (0, 2), (0, 3), (1, 2), (1, 3), (2, 3))
OTHERS = tuple(tuple(d for d in range(4) if d != face) for face in range(3))


def comp(direction, part, row, col):
    return ((direction * 2 + part) * 3 + row) * 3 + col


def face_comp(slot, part, row, col):
    return ((slot * 2 + part) * 2 + row) * 3 + col


def accumulate(terms):
    total = None
    for sign, left, right in terms:
        product = left * right
        if total is None:
            total = product if sign > 0 else -product
        else:
            total = total + product if sign > 0 else total - product
    return total


def product_rows(left, right):
    out = []
    for row in left:
        cols = []
        for j in range(3):
            re = accumulate(
                [(1, row[k][0], right[k][j][0]) for k in range(3)]
                + [(-1, row[k][1], right[k][j][1]) for k in range(3)]
            )
            im = accumulate(
                [(1, row[k][0], right[k][j][1]) for k in range(3)]
                + [(1, row[k][1], right[k][j][0]) for k in range(3)]
            )
            cols.append((re, im))
        out.append(cols)
    return out


def product_rows_dagger(left, right):
    out = []
    for row in left:
        cols = []
        for j in range(3):
            re = accumulate(
                [(1, row[k][0], right[j][k][0]) for k in range(3)]
                + [(1, row[k][1], right[j][k][1]) for k in range(3)]
            )
            im = accumulate(
                [(1, row[k][1], right[j][k][0]) for k in range(3)]
                + [(-1, row[k][0], right[j][k][1]) for k in range(3)]
            )
            cols.append((re, im))
        out.append(cols)
    return out


def cross_real(row0, row1, j):
    a, b = (j + 1) % 3, (j + 2) % 3
    return accumulate(
        [
            (1, row0[a][0], row1[b][0]),
            (-1, row0[a][1], row1[b][1]),
            (-1, row0[b][0], row1[a][0]),
            (1, row0[b][1], row1[a][1]),
        ]
    )


def cross_imag(row0, row1, j):
    a, b = (j + 1) % 3, (j + 2) % 3
    return accumulate(
        [
            (1, row0[b][0], row1[a][1]),
            (1, row0[b][1], row1[a][0]),
            (-1, row0[a][0], row1[b][1]),
            (-1, row0[a][1], row1[b][0]),
        ]
    )


def third_row(row0, row1):
    return [(cross_real(row0, row1, j), cross_imag(row0, row1, j)) for j in range(3)]


def plaquette(left, left_ahead, right, right_ahead):
    first = product_rows(left[:2], left_ahead)
    second = product_rows(right[:2], right_ahead)
    second.append(third_row(second[0], second[1]))
    loop = product_rows_dagger(first, second)
    row0, row1 = loop
    re20 = cross_real(row0, row1, 0)
    im20 = cross_imag(row0, row1, 0)
    re21 = cross_real(row0, row1, 1)
    im21 = cross_imag(row0, row1, 1)
    im22 = cross_imag(row0, row1, 2)
    third = (row0[0][1] + row1[1][1] + im22) * (1.0 / 3.0)
    d0 = row0[0][1] - third
    d1 = row1[1][1] - third
    return [
        row0[1][0] - row1[0][0],
        row0[1][1] + row1[0][1],
        row0[2][0] - re20,
        row0[2][1] + im20,
        row1[2][0] - re21,
        row1[2][1] + im21,
        d0 + d0,
        d1 + d1,
    ]


def rotated(force, link):
    r01, i01, r02, i02, r12, i12, d0, d1 = force
    d2 = -(d0 + d1)
    diag = (d0, d1, d2)
    upper = {(0, 1): (r01, i01), (0, 2): (r02, i02), (1, 2): (r12, i12)}
    columns = []
    for j in range(3):
        entries = []
        for k in range(3):
            re_terms = [(-1, diag[k], link[k][j][1])]
            im_terms = [(1, diag[k], link[k][j][0])]
            for l in range(3):
                if l == k:
                    continue
                if l > k:
                    re, im = upper[(k, l)]
                    sign = 1
                else:
                    re, im = upper[(l, k)]
                    sign = -1
                re_terms = [(sign, re, link[l][j][0])] + re_terms + [(-1, im, link[l][j][1])]
                im_terms = [(1, im, link[l][j][0])] + im_terms + [(sign, re, link[l][j][1])]
            re_terms.sort(key=lambda term: -term[0])
            entries.append((accumulate(re_terms), accumulate(im_terms)))
        columns.append(entries)

    def real(i, j):
        return accumulate(
            [(1, link[k][i][0], columns[j][k][0]) for k in range(3)]
            + [(1, link[k][i][1], columns[j][k][1]) for k in range(3)]
        )

    def imag(i, j):
        return accumulate(
            [(1, link[k][i][0], columns[j][k][1]) for k in range(3)]
            + [(-1, link[k][i][1], columns[j][k][0]) for k in range(3)]
        )

    return [real(0, 1), imag(0, 1), real(0, 2), imag(0, 2), real(1, 2), imag(1, 2), imag(0, 0), imag(1, 1)]


def lane_group(shape):
    return lax.broadcasted_iota(jnp.int32, shape, 1) // NX


def row_index(shape):
    return lax.broadcasted_iota(jnp.int32, shape, 0)


def turned(value, groups):
    return pltpu.roll(value, groups % 8 * NX, 1) if groups % 8 else value


def packed(values, last):
    total = None
    for group, value in enumerate(values):
        value = turned(value, group + 1 if last else group)
        total = value if total is None else jnp.where(lane_group(value.shape) == group, value, total)
    return total


def unpacked(value, group, last):
    return turned(value, 7 - group if last else -group)


def send_kernel(links, time_out, depth_out, plane_out):
    for face, out in ((0, time_out), (1, depth_out)):
        for slot, direction in enumerate(OTHERS[face]):
            for part in range(2):
                for row in range(2):
                    for col in range(3):
                        source = comp(direction, part, row, col)
                        target = face_comp(slot, part, row, col) * 4
                        if face == 0:
                            out[target : target + 4] = links[source, 0:DEPTHS]
                        else:
                            out[target : target + 4] = links[source, pl.ds(0, TIMES, stride=DEPTHS)]
    for part in range(2):
        for row in range(2):
            for col in range(3):
                target = ((part * 2 + row) * 3 + col) * 8
                plane_out[target : target + 8] = packed(
                    [
                        links[comp(direction, part, row, col), 8 * half : 8 * half + 8]
                        for half in range(2)
                        for direction in OTHERS[2]
                    ],
                    False,
                )


def matrix(ref, base, rows):
    return [
        [(ref[base + row * 3 + col, rows], ref[base + 9 + row * 3 + col, rows]) for col in range(3)]
        for row in range(3)
    ]


def face_matrix(ref, slot, size):
    rows = [
        [
            tuple(
                ref[face_comp(slot, part, row, col) * size : (face_comp(slot, part, row, col) + 1) * size]
                for part in range(2)
            )
            for col in range(3)
        ]
        for row in range(2)
    ]
    rows.append(third_row(rows[0], rows[1]))
    return rows


def shift_links(links, time_in, depth_in, plane_in, shifted):
    column = lax.broadcasted_iota(jnp.int32, (8, LANES), 1) % NX
    right_edge = column == NX - 1
    last_plane = lane_group((8, LANES)) == LANES // NX - 1
    for face in range(2):
        received = time_in if face == 0 else depth_in
        for slot, direction in enumerate(OTHERS[face]):
            halo = face_matrix(received, slot, 4)
            for part in range(2):
                for row in range(3):
                    for col in range(3):
                        c = comp(direction, part, row, col)
                        if face == 0:
                            shifted[0, c, 0 : ROWS - 4] = links[c, 4:ROWS]
                            shifted[0, c, ROWS - 4 : ROWS] = halo[row][col][part]
                        else:
                            shifted[1, c, 0 : ROWS - 1] = links[c, 1:ROWS]
                            shifted[1, c, pl.ds(3, TIMES, stride=DEPTHS)] = halo[row][col][part]
    halo = face_matrix(plane_in, 0, 8)
    for part in range(2):
        for row in range(3):
            for col in range(3):
                for slot, direction in enumerate(OTHERS[2]):
                    c = comp(direction, part, row, col)
                    for half in range(2):
                        rows = slice(8 * half, 8 * half + 8)
                        outer = unpacked(halo[row][col][part], 3 * half + slot, True)
                        shifted[2, c, rows] = jnp.where(last_plane, outer, turned(links[c, rows], 7))
    for direction in range(3):
        for offset in range(18):
            c = direction * 18 + offset
            for half in range(2):
                rows = slice(8 * half, 8 * half + 8)
                value = links[c, rows]
                shifted[3, c, rows] = jnp.where(
                    right_edge, pltpu.roll(value, NX - 1, 1), pltpu.roll(value, LANES - 1, 1)
                )


def interior_kernel(links, time_in, depth_in, plane_in, force, shifted, moved):
    shift_links(links, time_in, depth_in, plane_in, shifted)
    for face in range(2):
        for c in range(24):
            moved[face, c, 0:8] = jnp.zeros((8, LANES), jnp.float32)

    def step(half, carry):
        start = pl.multiple_of(half * 8, 8)
        rows = pl.ds(start, 8)
        column = lax.broadcasted_iota(jnp.int32, (8, LANES), 1)
        left_edge = column % NX == 0
        first_plane = column < NX
        fresh = [True] * 4

        def add(direction, values, sign):
            for i in range(8):
                c = direction * 8 + i
                if fresh[direction]:
                    force[c, rows] = values[i] if sign > 0 else -values[i]
                elif sign > 0:
                    force[c, rows] = force[c, rows] + values[i]
                else:
                    force[c, rows] = force[c, rows] - values[i]
            fresh[direction] = False

        def carry_over(direction, step_direction, values, sign):
            if step_direction < 2:
                slot = OTHERS[step_direction].index(direction)
                lower = pl.ds(pl.multiple_of(start + 8, 8), 8)
                for i in range(8):
                    moved[step_direction, slot * 8 + i, lower] = values[i] if sign > 0 else -values[i]
                return
            if step_direction == 2:
                values = [jnp.where(first_plane, 0.0, turned(v, 1)) for v in values]
            else:
                values = [
                    jnp.where(left_edge, pltpu.roll(v, LANES - NX + 1, 1), pltpu.roll(v, 1, 1))
                    for v in values
                ]
            add(direction, values, sign)

        for mu, nu in PAIRS:
            link_mu = matrix(links, mu * 18, rows)
            link_nu = matrix(links, nu * 18, rows)
            values = plaquette(
                link_mu,
                matrix(shifted.at[mu], nu * 18, rows),
                link_nu,
                matrix(shifted.at[nu], mu * 18, rows),
            )
            add(mu, values, 1)
            add(nu, values, -1)
            carry_over(mu, nu, rotated(values, link_nu), -1)
            carry_over(nu, mu, rotated(values, link_mu), 1)
        return carry

    lax.fori_loop(0, 2, step, 0)

    inner = row_index((8, LANES)) % DEPTHS != 0
    for direction in range(4):
        for i in range(8):
            c = direction * 8 + i
            for half in range(2):
                rows = slice(8 * half, 8 * half + 8)
                total = force[c, rows]
                if direction != 0:
                    slot = OTHERS[0].index(direction) * 8 + i
                    total = total + moved[0, slot, 8 * half + 4 : 8 * half + 12]
                if direction != 1:
                    slot = OTHERS[1].index(direction) * 8 + i
                    total = total + jnp.where(inner, moved[1, slot, 8 * half + 7 : 8 * half + 15], 0.0)
                force[c, rows] = total


def cells():
    return [(part, row, col) for part in range(2) for row in range(2) for col in range(3)]


def top(ref, face, c):
    return ref[c, 12:16] if face == 0 else ref[c, pl.ds(3, TIMES, stride=DEPTHS)]


def x_ahead(value):
    right_edge = lax.broadcasted_iota(jnp.int32, value.shape, 1) % NX == NX - 1
    return jnp.where(right_edge, pltpu.roll(value, NX - 1, 1), pltpu.roll(value, LANES - 1, 1))


def prepare_kernel(links, left, ahead, base):
    for part in range(2):
        for row in range(3):
            for col in range(3):
                at = part * 9 + row * 3 + col
                base[0, at, 0:4] = top(links, 0, comp(0, part, row, col))
                base[0, at, 4:8] = top(links, 1, comp(1, part, row, col))
                c = comp(2, part, row, col)
                base[1, at] = packed([links[c, 8 * (q // 3) : 8 * (q // 3) + 8] for q in range(6)], True)
    for part, row, col in cells():
        at = face_comp(0, part, row, col)
        whole = part * 9 + row * 3 + col
        for unit in range(3):
            for face in range(2):
                source = comp(OTHERS[face][unit], part, row, col)
                left[unit, at, 4 * face : 4 * face + 4] = top(links, face, source)
        left[3, at] = packed(
            [
                links[comp(direction, part, row, col), 8 * half : 8 * half + 8]
                for half in range(2)
                for direction in OTHERS[2]
            ],
            True,
        )
        ahead[0, at] = jnp.zeros((8, LANES), jnp.float32)
        ahead[0, at, 0:3] = links[comp(0, part, row, col), 13:16]
        ahead[0, at, 4:7] = links[comp(1, part, row, col), pl.ds(7, 3, stride=DEPTHS)]
        ahead[1, at] = turned(base[0, whole], 7)
        ahead[2, at] = x_ahead(base[0, whole])
        c = comp(2, part, row, col)
        upper = links[c, 8:16]
        along_x = x_ahead(base[1, whole])
        group = lane_group((8, LANES))
        for q, value in (
            (0, links[c, 4:12]),
            (1, links[c, 1:9]),
            (3, pltpu.roll(upper, 4, 0)),
            (4, pltpu.roll(upper, 7, 0)),
        ):
            along_x = jnp.where(group == q, turned(value, q + 1), along_x)
        ahead[3, at] = along_x


def wide(ref, row):
    return jnp.broadcast_to(ref[row : row + 1], (8, LANES))


def boundary_kernel(left, ahead, base, time_in, depth_in, plane_in, time_out, depth_out, plane_out):
    row_at = row_index((8, LANES))
    group = lane_group((8, LANES))

    def behind(unit, part, row, col):
        if unit == 3:
            at = face_comp(0, part, row, col) * 8
            return plane_in[at : at + 8]
        at = face_comp(unit, part, row, col) * 4
        return jnp.concatenate([time_in[at : at + 4], depth_in[at : at + 4]], axis=0)

    def beside(unit, part, row, col):
        at = face_comp(0, part, row, col)
        own = ahead[unit, at]
        if unit == 0:
            own = jnp.where(row_at == 3, wide(depth_in, at * 4 + 3), own)
            return jnp.where(row_at == 7, wide(time_in, at * 4 + 3), own)
        if unit == 1:
            time_part = turned(pltpu.roll(plane_in[at * 8 : at * 8 + 8], 4, 0), 4)
            depth_part = jnp.where(row_at % 2 == 1, wide(plane_in, at * 8 + 7), wide(plane_in, at * 8 + 3))
            depth_part = jnp.where(row_at < 6, turned(depth_part, 6), turned(depth_part, 3))
            return jnp.where(group == 7, jnp.where(row_at < 4, time_part, depth_part), own)
        if unit == 2:
            return own
        source = face_comp(1, part, row, col) * 4
        later = turned(time_in[source - 4 : source + 4], 4)
        own = jnp.where((group == 3) & (row_at >= 4), later, own)
        for half in range(2):
            first, second = wide(depth_in, source + 2 * half), wide(depth_in, source + 2 * half + 1)
            q = 3 * half + 1
            deeper = turned(jnp.where(row_at < 4, first, second), q + 1)
            own = jnp.where((group == q) & (row_at % 4 == 3), deeper, own)
        return own

    def complete(fetch):
        rows = [[(fetch(0, row, col), fetch(1, row, col)) for col in range(3)] for row in range(2)]
        rows.append(third_row(rows[0], rows[1]))
        return rows

    for unit in range(4):
        own_base = [
            [tuple(base[unit // 3, part * 9 + row * 3 + col] for part in range(2)) for col in range(3)]
            for row in range(3)
        ]
        own_left = [
            [tuple(left[unit, face_comp(0, part, row, col)] for part in range(2)) for col in range(3)]
            for row in range(2)
        ]
        values = plaquette(
            own_left,
            complete(lambda part, row, col: beside(unit, part, row, col)),
            own_base,
            complete(lambda part, row, col: behind(unit, part, row, col)),
        )
        for i, value in enumerate(rotated(values, own_base)):
            if unit == 3:
                plane_out[8 * i : 8 * i + 8] = value
            else:
                at = (unit * 8 + i) * 4
                time_out[at : at + 4] = value[0:4]
                depth_out[at : at + 4] = value[4:8]


def final_kernel(force, time_in, depth_in, plane_in, out, work):
    first_plane = lax.broadcasted_iota(jnp.int32, (8, LANES), 1) < NX
    for direction in range(4):
        for i in range(8):
            c = direction * 8 + i
            for half in range(2):
                rows = slice(8 * half, 8 * half + 8)
                total = force[c, rows]
                if direction != 2:
                    group = 3 * half + OTHERS[2].index(direction)
                    outer = unpacked(plane_in[8 * i : 8 * i + 8], group, False)
                    total = total - jnp.where(first_plane, outer, 0.0)
                work[c, rows] = total
            if direction != 0:
                at = (OTHERS[0].index(direction) * 8 + i) * 4
                work[c, 0:4] = work[c, 0:4] - time_in[at : at + 4]
            if direction != 1:
                at = (OTHERS[1].index(direction) * 8 + i) * 4
                sites = pl.ds(0, TIMES, stride=DEPTHS)
                work[c, sites] = work[c, sites] - depth_in[at : at + 4]
        half_coeff = 0.5 * COEFF
        upper = ((0, 1), (0, 2), (1, 2))
        for half in range(2):
            rows = slice(8 * half, 8 * half + 8)
            for n, (row, col) in enumerate(upper):
                re = work[direction * 8 + 2 * n, rows] * half_coeff
                im = work[direction * 8 + 2 * n + 1, rows] * half_coeff
                out[comp(direction, 0, row, col), rows] = re
                out[comp(direction, 0, col, row), rows] = -re
                out[comp(direction, 1, row, col), rows] = im
                out[comp(direction, 1, col, row), rows] = im
            d0 = work[direction * 8 + 6, rows] * half_coeff
            d1 = work[direction * 8 + 7, rows] * half_coeff
            zero = jnp.zeros_like(d0)
            for k, value in enumerate((d0, d1, -(d0 + d1))):
                out[comp(direction, 1, k, k), rows] = value
                out[comp(direction, 0, k, k), rows] = zero


def shape(*dims):
    return pltpu.VMEM(dims, jnp.float32)


def move(value, axis, forward):
    count = lax.axis_size(axis)
    step = 1 if forward else count - 1
    moved = lax.ppermute(value, axis, [(i, (i + step) % count) for i in range(count)])
    return pltpu.with_memory_space_constraint(moved, pltpu.VMEM)


def gauge_force(links):
    flat = pltpu.with_memory_space_constraint(links.reshape(72, ROWS, LANES), pltpu.VMEM)
    faces = pl.pallas_call(
        send_kernel, out_shape=(shape(144, LANES), shape(144, LANES), shape(96, LANES)), name="send"
    )(flat)
    depth = move(faces[1], "gz", False)
    time = move(faces[0], "ta", False)
    plane = move(faces[2], "gx", False)
    local = pl.pallas_call(
        prepare_kernel,
        out_shape=(shape(4, 12, 8, LANES), shape(4, 12, 8, LANES), shape(2, 18, 8, LANES)),
        name="prepare",
    )(flat)
    local = [pltpu.with_memory_space_constraint(value, pltpu.VMEM) for value in local]
    sent = pl.pallas_call(
        boundary_kernel,
        out_shape=(shape(96, LANES), shape(96, LANES), shape(64, LANES)),
        name="boundary",
    )(*local, time, depth, plane)
    force = pl.pallas_call(
        interior_kernel,
        out_shape=shape(32, ROWS, LANES),
        scratch_shapes=[
            pltpu.VMEM((4, 72, ROWS, LANES), jnp.float32),
            pltpu.VMEM((2, 24, 24, LANES), jnp.float32),
        ],
        name="interior",
    )(flat, time, depth, plane)
    depth = move(sent[1], "gz", True)
    time = move(sent[0], "ta", True)
    plane = move(sent[2], "gx", True)
    out = pl.pallas_call(
        final_kernel,
        out_shape=jax.ShapeDtypeStruct((72, ROWS, LANES), jnp.float32),
        scratch_shapes=[pltpu.VMEM((32, ROWS, LANES), jnp.float32)],
        name="final",
    )(pltpu.with_memory_space_constraint(force, pltpu.VMEM), time, depth, plane)
    return out.reshape(links.shape)


def solution(mesh):
    spec = P(None, None, None, None, "ta", "gz", "gx")
    return jax.shard_map(gauge_force, mesh=mesh, in_specs=(spec,), out_specs=spec, check_vma=False)
```

```python
import jax
import jax.numpy as jnp
from jax import lax
from jax.experimental import pallas as pl
from jax.experimental.pallas import tpu as pltpu
from jax.sharding import PartitionSpec as P


NX = 16
COEFF = -1.9

ROWS = 16
LANES = 128
TIMES = 4
DEPTHS = 4
PAIRS = ((0, 1), (0, 2), (0, 3), (1, 2), (1, 3), (2, 3))
OTHERS = tuple(tuple(d for d in range(4) if d != face) for face in range(3))


def comp(direction, part, row, col):
    return ((direction * 2 + part) * 3 + row) * 3 + col


def face_comp(slot, part, row, col):
    return ((slot * 2 + part) * 2 + row) * 3 + col


def accumulate(terms):
    total = None
    for sign, left, right in terms:
        product = left * right
        if total is None:
            total = product if sign > 0 else -product
        else:
            total = total + product if sign > 0 else total - product
    return total


def product_rows(left, right):
    out = []
    for row in left:
        cols = []
        for j in range(3):
            re = accumulate(
                [(1, row[k][0], right[k][j][0]) for k in range(3)]
                + [(-1, row[k][1], right[k][j][1]) for k in range(3)]
            )
            im = accumulate(
                [(1, row[k][0], right[k][j][1]) for k in range(3)]
                + [(1, row[k][1], right[k][j][0]) for k in range(3)]
            )
            cols.append((re, im))
        out.append(cols)
    return out


def product_rows_dagger(left, right):
    out = []
    for row in left:
        cols = []
        for j in range(3):
            re = accumulate(
                [(1, row[k][0], right[j][k][0]) for k in range(3)]
                + [(1, row[k][1], right[j][k][1]) for k in range(3)]
            )
            im = accumulate(
                [(1, row[k][1], right[j][k][0]) for k in range(3)]
                + [(-1, row[k][0], right[j][k][1]) for k in range(3)]
            )
            cols.append((re, im))
        out.append(cols)
    return out


def cross_real(row0, row1, j):
    a, b = (j + 1) % 3, (j + 2) % 3
    return accumulate(
        [
            (1, row0[a][0], row1[b][0]),
            (-1, row0[a][1], row1[b][1]),
            (-1, row0[b][0], row1[a][0]),
            (1, row0[b][1], row1[a][1]),
        ]
    )


def cross_imag(row0, row1, j):
    a, b = (j + 1) % 3, (j + 2) % 3
    return accumulate(
        [
            (1, row0[b][0], row1[a][1]),
            (1, row0[b][1], row1[a][0]),
            (-1, row0[a][0], row1[b][1]),
            (-1, row0[a][1], row1[b][0]),
        ]
    )


def third_row(row0, row1):
    return [(cross_real(row0, row1, j), cross_imag(row0, row1, j)) for j in range(3)]


def plaquette(left, left_ahead, right, right_ahead):
    first = product_rows(left[:2], left_ahead)
    second = product_rows(right[:2], right_ahead)
    second.append(third_row(second[0], second[1]))
    loop = product_rows_dagger(first, second)
    row0, row1 = loop
    re20 = cross_real(row0, row1, 0)
    im20 = cross_imag(row0, row1, 0)
    re21 = cross_real(row0, row1, 1)
    im21 = cross_imag(row0, row1, 1)
    im22 = cross_imag(row0, row1, 2)
    third = (row0[0][1] + row1[1][1] + im22) * (1.0 / 3.0)
    d0 = row0[0][1] - third
    d1 = row1[1][1] - third
    return [
        row0[1][0] - row1[0][0],
        row0[1][1] + row1[0][1],
        row0[2][0] - re20,
        row0[2][1] + im20,
        row1[2][0] - re21,
        row1[2][1] + im21,
        d0 + d0,
        d1 + d1,
    ]


def rotated(force, link):
    r01, i01, r02, i02, r12, i12, d0, d1 = force
    d2 = -(d0 + d1)
    diag = (d0, d1, d2)
    upper = {(0, 1): (r01, i01), (0, 2): (r02, i02), (1, 2): (r12, i12)}
    columns = []
    for j in range(3):
        entries = []
        for k in range(3):
            re_terms = [(-1, diag[k], link[k][j][1])]
            im_terms = [(1, diag[k], link[k][j][0])]
            for l in range(3):
                if l == k:
                    continue
                if l > k:
                    re, im = upper[(k, l)]
                    sign = 1
                else:
                    re, im = upper[(l, k)]
                    sign = -1
                re_terms = [(sign, re, link[l][j][0])] + re_terms + [(-1, im, link[l][j][1])]
                im_terms = [(1, im, link[l][j][0])] + im_terms + [(sign, re, link[l][j][1])]
            re_terms.sort(key=lambda term: -term[0])
            entries.append((accumulate(re_terms), accumulate(im_terms)))
        columns.append(entries)

    def real(i, j):
        return accumulate(
            [(1, link[k][i][0], columns[j][k][0]) for k in range(3)]
            + [(1, link[k][i][1], columns[j][k][1]) for k in range(3)]
        )

    def imag(i, j):
        return accumulate(
            [(1, link[k][i][0], columns[j][k][1]) for k in range(3)]
            + [(-1, link[k][i][1], columns[j][k][0]) for k in range(3)]
        )

    return [real(0, 1), imag(0, 1), real(0, 2), imag(0, 2), real(1, 2), imag(1, 2), imag(0, 0), imag(1, 1)]


def lane_group(shape):
    return lax.broadcasted_iota(jnp.int32, shape, 1) // NX


def row_index(shape):
    return lax.broadcasted_iota(jnp.int32, shape, 0)


def turned(value, groups):
    return pltpu.roll(value, groups % 8 * NX, 1) if groups % 8 else value


def packed(values, last):
    total = None
    for group, value in enumerate(values):
        value = turned(value, group + 1 if last else group)
        total = value if total is None else jnp.where(lane_group(value.shape) == group, value, total)
    return total


def unpacked(value, group, last):
    return turned(value, 7 - group if last else -group)


def send_kernel(links, time_out, depth_out, plane_out):
    for face, out in ((0, time_out), (1, depth_out)):
        for slot, direction in enumerate(OTHERS[face]):
            for part in range(2):
                for row in range(2):
                    for col in range(3):
                        source = comp(direction, part, row, col)
                        target = face_comp(slot, part, row, col) * 4
                        if face == 0:
                            out[target : target + 4] = links[source, 0:DEPTHS]
                        else:
                            out[target : target + 4] = links[source, pl.ds(0, TIMES, stride=DEPTHS)]
    for part in range(2):
        for row in range(2):
            for col in range(3):
                target = ((part * 2 + row) * 3 + col) * 8
                plane_out[target : target + 8] = packed(
                    [
                        links[comp(direction, part, row, col), 8 * half : 8 * half + 8]
                        for half in range(2)
                        for direction in OTHERS[2]
                    ],
                    False,
                )


def matrix(ref, base, rows):
    return [
        [(ref[base + row * 3 + col, rows], ref[base + 9 + row * 3 + col, rows]) for col in range(3)]
        for row in range(3)
    ]


def face_matrix(ref, slot, size):
    rows = [
        [
            tuple(
                ref[face_comp(slot, part, row, col) * size : (face_comp(slot, part, row, col) + 1) * size]
                for part in range(2)
            )
            for col in range(3)
        ]
        for row in range(2)
    ]
    rows.append(third_row(rows[0], rows[1]))
    return rows


def shift_links(links, time_in, depth_in, plane_in, shifted):
    column = lax.broadcasted_iota(jnp.int32, (8, LANES), 1) % NX
    right_edge = column == NX - 1
    last_plane = lane_group((8, LANES)) == LANES // NX - 1
    for face in range(2):
        received = time_in if face == 0 else depth_in
        for slot, direction in enumerate(OTHERS[face]):
            halo = face_matrix(received, slot, 4)
            for part in range(2):
                for row in range(3):
                    for col in range(3):
                        c = comp(direction, part, row, col)
                        if face == 0:
                            shifted[0, c, 0 : ROWS - 4] = links[c, 4:ROWS]
                            shifted[0, c, ROWS - 4 : ROWS] = halo[row][col][part]
                        else:
                            shifted[1, c, 0 : ROWS - 1] = links[c, 1:ROWS]
                            shifted[1, c, pl.ds(3, TIMES, stride=DEPTHS)] = halo[row][col][part]
    halo = face_matrix(plane_in, 0, 8)
    for part in range(2):
        for row in range(3):
            for col in range(3):
                for slot, direction in enumerate(OTHERS[2]):
                    c = comp(direction, part, row, col)
                    for half in range(2):
                        rows = slice(8 * half, 8 * half + 8)
                        outer = unpacked(halo[row][col][part], 3 * half + slot, True)
                        shifted[2, c, rows] = jnp.where(last_plane, outer, turned(links[c, rows], 7))
    for direction in range(3):
        for offset in range(18):
            c = direction * 18 + offset
            for half in range(2):
                rows = slice(8 * half, 8 * half + 8)
                value = links[c, rows]
                shifted[3, c, rows] = jnp.where(
                    right_edge, pltpu.roll(value, NX - 1, 1), pltpu.roll(value, LANES - 1, 1)
                )


def interior_kernel(links, time_in, depth_in, plane_in, force, shifted, moved):
    shift_links(links, time_in, depth_in, plane_in, shifted)
    for face in range(2):
        for c in range(24):
            moved[face, c, 0:8] = jnp.zeros((8, LANES), jnp.float32)

    def step(half, carry):
        start = pl.multiple_of(half * 8, 8)
        rows = pl.ds(start, 8)
        column = lax.broadcasted_iota(jnp.int32, (8, LANES), 1)
        left_edge = column % NX == 0
        first_plane = column < NX
        fresh = [True] * 4

        def add(direction, values, sign):
            for i in range(8):
                c = direction * 8 + i
                if fresh[direction]:
                    force[c, rows] = values[i] if sign > 0 else -values[i]
                elif sign > 0:
                    force[c, rows] = force[c, rows] + values[i]
                else:
                    force[c, rows] = force[c, rows] - values[i]
            fresh[direction] = False

        def carry_over(direction, step_direction, values, sign):
            if step_direction < 2:
                slot = OTHERS[step_direction].index(direction)
                lower = pl.ds(pl.multiple_of(start + 8, 8), 8)
                for i in range(8):
                    moved[step_direction, slot * 8 + i, lower] = values[i] if sign > 0 else -values[i]
                return
            if step_direction == 2:
                values = [jnp.where(first_plane, 0.0, turned(v, 1)) for v in values]
            else:
                values = [
                    jnp.where(left_edge, pltpu.roll(v, LANES - NX + 1, 1), pltpu.roll(v, 1, 1))
                    for v in values
                ]
            add(direction, values, sign)

        for mu, nu in PAIRS:
            link_mu = matrix(links, mu * 18, rows)
            link_nu = matrix(links, nu * 18, rows)
            values = plaquette(
                link_mu,
                matrix(shifted.at[mu], nu * 18, rows),
                link_nu,
                matrix(shifted.at[nu], mu * 18, rows),
            )
            add(mu, values, 1)
            add(nu, values, -1)
            carry_over(mu, nu, rotated(values, link_nu), -1)
            carry_over(nu, mu, rotated(values, link_mu), 1)
        return carry

    lax.fori_loop(0, 2, step, 0)

    inner = row_index((8, LANES)) % DEPTHS != 0
    for direction in range(4):
        for i in range(8):
            c = direction * 8 + i
            for half in range(2):
                rows = slice(8 * half, 8 * half + 8)
                total = force[c, rows]
                if direction != 0:
                    slot = OTHERS[0].index(direction) * 8 + i
                    total = total + moved[0, slot, 8 * half + 4 : 8 * half + 12]
                if direction != 1:
                    slot = OTHERS[1].index(direction) * 8 + i
                    total = total + jnp.where(inner, moved[1, slot, 8 * half + 7 : 8 * half + 15], 0.0)
                force[c, rows] = total


def cells():
    return [(part, row, col) for part in range(2) for row in range(2) for col in range(3)]


def top(ref, face, c):
    return ref[c, 12:16] if face == 0 else ref[c, pl.ds(3, TIMES, stride=DEPTHS)]


def x_ahead(value):
    right_edge = lax.broadcasted_iota(jnp.int32, value.shape, 1) % NX == NX - 1
    return jnp.where(right_edge, pltpu.roll(value, NX - 1, 1), pltpu.roll(value, LANES - 1, 1))


def prepare_kernel(links, left, ahead, base):
    for part in range(2):
        for row in range(3):
            for col in range(3):
                at = part * 9 + row * 3 + col
                base[0, at, 0:4] = top(links, 0, comp(0, part, row, col))
                base[0, at, 4:8] = top(links, 1, comp(1, part, row, col))
                c = comp(2, part, row, col)
                base[1, at] = packed([links[c, 8 * (q // 3) : 8 * (q // 3) + 8] for q in range(6)], True)
    for part, row, col in cells():
        at = face_comp(0, part, row, col)
        whole = part * 9 + row * 3 + col
        for unit in range(3):
            for face in range(2):
                source = comp(OTHERS[face][unit], part, row, col)
                left[unit, at, 4 * face : 4 * face + 4] = top(links, face, source)
        left[3, at] = packed(
            [
                links[comp(direction, part, row, col), 8 * half : 8 * half + 8]
                for half in range(2)
                for direction in OTHERS[2]
            ],
            True,
        )
        ahead[0, at] = jnp.zeros((8, LANES), jnp.float32)
        ahead[0, at, 0:3] = links[comp(0, part, row, col), 13:16]
        ahead[0, at, 4:7] = links[comp(1, part, row, col), pl.ds(7, 3, stride=DEPTHS)]
        ahead[1, at] = turned(base[0, whole], 7)
        ahead[2, at] = x_ahead(base[0, whole])
        c = comp(2, part, row, col)
        upper = links[c, 8:16]
        along_x = x_ahead(base[1, whole])
        group = lane_group((8, LANES))
        for q, value in (
            (0, links[c, 4:12]),
            (1, links[c, 1:9]),
            (3, pltpu.roll(upper, 4, 0)),
            (4, pltpu.roll(upper, 7, 0)),
        ):
            along_x = jnp.where(group == q, turned(value, q + 1), along_x)
        ahead[3, at] = along_x


def wide(ref, row):
    return jnp.broadcast_to(ref[row : row + 1], (8, LANES))


def faces_kernel(left, ahead, base, time_in, depth_in, plane_in, time_out, depth_out):
    boundary((0, 1, 2), left, ahead, base, time_in, depth_in, plane_in, time_out, depth_out, None)


def plane_kernel(left, ahead, base, time_in, depth_in, plane_in, plane_out):
    boundary((3,), left, ahead, base, time_in, depth_in, plane_in, None, None, plane_out)


def boundary(units, left, ahead, base, time_in, depth_in, plane_in, time_out, depth_out, plane_out):
    row_at = row_index((8, LANES))
    group = lane_group((8, LANES))

    def behind(unit, part, row, col):
        if unit == 3:
            at = face_comp(0, part, row, col) * 8
            return plane_in[at : at + 8]
        at = face_comp(unit, part, row, col) * 4
        return jnp.concatenate([time_in[at : at + 4], depth_in[at : at + 4]], axis=0)

    def beside(unit, part, row, col):
        at = face_comp(0, part, row, col)
        own = ahead[unit, at]
        if unit == 0:
            own = jnp.where(row_at == 3, wide(depth_in, at * 4 + 3), own)
            return jnp.where(row_at == 7, wide(time_in, at * 4 + 3), own)
        if unit == 1:
            time_part = turned(pltpu.roll(plane_in[at * 8 : at * 8 + 8], 4, 0), 4)
            depth_part = jnp.where(row_at % 2 == 1, wide(plane_in, at * 8 + 7), wide(plane_in, at * 8 + 3))
            depth_part = jnp.where(row_at < 6, turned(depth_part, 6), turned(depth_part, 3))
            return jnp.where(group == 7, jnp.where(row_at < 4, time_part, depth_part), own)
        if unit == 2:
            return own
        source = face_comp(1, part, row, col) * 4
        later = turned(time_in[source - 4 : source + 4], 4)
        own = jnp.where((group == 3) & (row_at >= 4), later, own)
        for half in range(2):
            first, second = wide(depth_in, source + 2 * half), wide(depth_in, source + 2 * half + 1)
            q = 3 * half + 1
            deeper = turned(jnp.where(row_at < 4, first, second), q + 1)
            own = jnp.where((group == q) & (row_at % 4 == 3), deeper, own)
        return own

    def complete(fetch):
        rows = [[(fetch(0, row, col), fetch(1, row, col)) for col in range(3)] for row in range(2)]
        rows.append(third_row(rows[0], rows[1]))
        return rows

    for unit in units:
        own_base = [
            [tuple(base[unit // 3, part * 9 + row * 3 + col] for part in range(2)) for col in range(3)]
            for row in range(3)
        ]
        own_left = [
            [tuple(left[unit, face_comp(0, part, row, col)] for part in range(2)) for col in range(3)]
            for row in range(2)
        ]
        values = plaquette(
            own_left,
            complete(lambda part, row, col: beside(unit, part, row, col)),
            own_base,
            complete(lambda part, row, col: behind(unit, part, row, col)),
        )
        for i, value in enumerate(rotated(values, own_base)):
            if unit == 3:
                plane_out[8 * i : 8 * i + 8] = value
            else:
                at = (unit * 8 + i) * 4
                time_out[at : at + 4] = value[0:4]
                depth_out[at : at + 4] = value[4:8]


def final_kernel(force, time_in, depth_in, plane_in, out, work):
    first_plane = lax.broadcasted_iota(jnp.int32, (8, LANES), 1) < NX
    for direction in range(4):
        for i in range(8):
            c = direction * 8 + i
            for half in range(2):
                rows = slice(8 * half, 8 * half + 8)
                total = force[c, rows]
                if direction != 2:
                    group = 3 * half + OTHERS[2].index(direction)
                    outer = unpacked(plane_in[8 * i : 8 * i + 8], group, False)
                    total = total - jnp.where(first_plane, outer, 0.0)
                work[c, rows] = total
            if direction != 0:
                at = (OTHERS[0].index(direction) * 8 + i) * 4
                work[c, 0:4] = work[c, 0:4] - time_in[at : at + 4]
            if direction != 1:
                at = (OTHERS[1].index(direction) * 8 + i) * 4
                sites = pl.ds(0, TIMES, stride=DEPTHS)
                work[c, sites] = work[c, sites] - depth_in[at : at + 4]
        half_coeff = 0.5 * COEFF
        upper = ((0, 1), (0, 2), (1, 2))
        for half in range(2):
            rows = slice(8 * half, 8 * half + 8)
            for n, (row, col) in enumerate(upper):
                re = work[direction * 8 + 2 * n, rows] * half_coeff
                im = work[direction * 8 + 2 * n + 1, rows] * half_coeff
                out[comp(direction, 0, row, col), rows] = re
                out[comp(direction, 0, col, row), rows] = -re
                out[comp(direction, 1, row, col), rows] = im
                out[comp(direction, 1, col, row), rows] = im
            d0 = work[direction * 8 + 6, rows] * half_coeff
            d1 = work[direction * 8 + 7, rows] * half_coeff
            zero = jnp.zeros_like(d0)
            for k, value in enumerate((d0, d1, -(d0 + d1))):
                out[comp(direction, 1, k, k), rows] = value
                out[comp(direction, 0, k, k), rows] = zero


def shape(*dims):
    return pltpu.VMEM(dims, jnp.float32)


def move(value, axis, forward):
    count = lax.axis_size(axis)
    step = 1 if forward else count - 1
    moved = lax.ppermute(value, axis, [(i, (i + step) % count) for i in range(count)])
    return pltpu.with_memory_space_constraint(moved, pltpu.VMEM)


def gauge_force(links):
    flat = pltpu.with_memory_space_constraint(links.reshape(72, ROWS, LANES), pltpu.VMEM)
    faces = pl.pallas_call(
        send_kernel, out_shape=(shape(144, LANES), shape(144, LANES), shape(96, LANES)), name="send"
    )(flat)
    depth = move(faces[1], "gz", False)
    time = move(faces[0], "ta", False)
    plane = move(faces[2], "gx", False)
    local = pl.pallas_call(
        prepare_kernel,
        out_shape=(shape(4, 12, 8, LANES), shape(4, 12, 8, LANES), shape(2, 18, 8, LANES)),
        name="prepare",
    )(flat)
    local = [pltpu.with_memory_space_constraint(value, pltpu.VMEM) for value in local]
    sent = pl.pallas_call(faces_kernel, out_shape=(shape(96, LANES), shape(96, LANES)), name="faces")(
        *local, time, depth, plane
    )
    sent_plane = pl.pallas_call(plane_kernel, out_shape=shape(64, LANES), name="plane")(
        *local, time, depth, plane
    )
    force = pl.pallas_call(
        interior_kernel,
        out_shape=shape(32, ROWS, LANES),
        scratch_shapes=[
            pltpu.VMEM((4, 72, ROWS, LANES), jnp.float32),
            pltpu.VMEM((2, 24, 24, LANES), jnp.float32),
        ],
        name="interior",
    )(flat, time, depth, plane)
    depth = move(sent[1], "gz", True)
    time = move(sent[0], "ta", True)
    plane = move(sent_plane, "gx", True)
    out = pl.pallas_call(
        final_kernel,
        out_shape=jax.ShapeDtypeStruct((72, ROWS, LANES), jnp.float32),
        scratch_shapes=[pltpu.VMEM((32, ROWS, LANES), jnp.float32)],
        name="final",
    )(pltpu.with_memory_space_constraint(force, pltpu.VMEM), time, depth, plane)
    return out.reshape(links.shape)


def solution(mesh):
    spec = P(None, None, None, None, "ta", "gz", "gx")
    return jax.shard_map(gauge_force, mesh=mesh, in_specs=(spec,), out_specs=spec, check_vma=False)
```

```python
import jax
import jax.numpy as jnp
from jax import lax
from jax.experimental import pallas as pl
from jax.experimental.pallas import tpu as pltpu
from jax.sharding import PartitionSpec as P


NX = 16
COEFF = -1.9

ROWS = 16
LANES = 128
TIMES = 4
DEPTHS = 4
PAIRS = ((0, 1), (0, 2), (0, 3), (1, 2), (1, 3), (2, 3))
OTHERS = tuple(tuple(d for d in range(4) if d != face) for face in range(3))


def comp(direction, part, row, col):
    return ((direction * 2 + part) * 3 + row) * 3 + col


def face_comp(slot, part, row, col):
    return ((slot * 2 + part) * 2 + row) * 3 + col


def accumulate(terms):
    total = None
    for sign, left, right in terms:
        product = left * right
        if total is None:
            total = product if sign > 0 else -product
        else:
            total = total + product if sign > 0 else total - product
    return total


def product_rows(left, right):
    out = []
    for row in left:
        cols = []
        for j in range(3):
            re = accumulate(
                [(1, row[k][0], right[k][j][0]) for k in range(3)]
                + [(-1, row[k][1], right[k][j][1]) for k in range(3)]
            )
            im = accumulate(
                [(1, row[k][0], right[k][j][1]) for k in range(3)]
                + [(1, row[k][1], right[k][j][0]) for k in range(3)]
            )
            cols.append((re, im))
        out.append(cols)
    return out


def product_rows_dagger(left, right):
    out = []
    for row in left:
        cols = []
        for j in range(3):
            re = accumulate(
                [(1, row[k][0], right[j][k][0]) for k in range(3)]
                + [(1, row[k][1], right[j][k][1]) for k in range(3)]
            )
            im = accumulate(
                [(1, row[k][1], right[j][k][0]) for k in range(3)]
                + [(-1, row[k][0], right[j][k][1]) for k in range(3)]
            )
            cols.append((re, im))
        out.append(cols)
    return out


def cross_real(row0, row1, j):
    a, b = (j + 1) % 3, (j + 2) % 3
    return accumulate(
        [
            (1, row0[a][0], row1[b][0]),
            (-1, row0[a][1], row1[b][1]),
            (-1, row0[b][0], row1[a][0]),
            (1, row0[b][1], row1[a][1]),
        ]
    )


def cross_imag(row0, row1, j):
    a, b = (j + 1) % 3, (j + 2) % 3
    return accumulate(
        [
            (1, row0[b][0], row1[a][1]),
            (1, row0[b][1], row1[a][0]),
            (-1, row0[a][0], row1[b][1]),
            (-1, row0[a][1], row1[b][0]),
        ]
    )


def third_row(row0, row1):
    return [(cross_real(row0, row1, j), cross_imag(row0, row1, j)) for j in range(3)]


def plaquette(left, left_ahead, right, right_ahead):
    first = product_rows(left[:2], left_ahead)
    second = product_rows(right[:2], right_ahead)
    second.append(third_row(second[0], second[1]))
    loop = product_rows_dagger(first, second)
    row0, row1 = loop
    re20 = cross_real(row0, row1, 0)
    im20 = cross_imag(row0, row1, 0)
    re21 = cross_real(row0, row1, 1)
    im21 = cross_imag(row0, row1, 1)
    im22 = cross_imag(row0, row1, 2)
    third = (row0[0][1] + row1[1][1] + im22) * (1.0 / 3.0)
    d0 = row0[0][1] - third
    d1 = row1[1][1] - third
    return [
        row0[1][0] - row1[0][0],
        row0[1][1] + row1[0][1],
        row0[2][0] - re20,
        row0[2][1] + im20,
        row1[2][0] - re21,
        row1[2][1] + im21,
        d0 + d0,
        d1 + d1,
    ]


def rotated(force, link):
    r01, i01, r02, i02, r12, i12, d0, d1 = force
    d2 = -(d0 + d1)
    diag = (d0, d1, d2)
    upper = {(0, 1): (r01, i01), (0, 2): (r02, i02), (1, 2): (r12, i12)}
    columns = []
    for j in range(3):
        entries = []
        for k in range(3):
            re_terms = [(-1, diag[k], link[k][j][1])]
            im_terms = [(1, diag[k], link[k][j][0])]
            for l in range(3):
                if l == k:
                    continue
                if l > k:
                    re, im = upper[(k, l)]
                    sign = 1
                else:
                    re, im = upper[(l, k)]
                    sign = -1
                re_terms = [(sign, re, link[l][j][0])] + re_terms + [(-1, im, link[l][j][1])]
                im_terms = [(1, im, link[l][j][0])] + im_terms + [(sign, re, link[l][j][1])]
            re_terms.sort(key=lambda term: -term[0])
            entries.append((accumulate(re_terms), accumulate(im_terms)))
        columns.append(entries)

    def real(i, j):
        return accumulate(
            [(1, link[k][i][0], columns[j][k][0]) for k in range(3)]
            + [(1, link[k][i][1], columns[j][k][1]) for k in range(3)]
        )

    def imag(i, j):
        return accumulate(
            [(1, link[k][i][0], columns[j][k][1]) for k in range(3)]
            + [(-1, link[k][i][1], columns[j][k][0]) for k in range(3)]
        )

    return [real(0, 1), imag(0, 1), real(0, 2), imag(0, 2), real(1, 2), imag(1, 2), imag(0, 0), imag(1, 1)]


def lane_group(shape):
    return lax.broadcasted_iota(jnp.int32, shape, 1) // NX


def row_index(shape):
    return lax.broadcasted_iota(jnp.int32, shape, 0)


def turned(value, groups):
    return pltpu.roll(value, groups % 8 * NX, 1) if groups % 8 else value


def packed(values, last):
    total = None
    for group, value in enumerate(values):
        value = turned(value, group + 1 if last else group)
        total = value if total is None else jnp.where(lane_group(value.shape) == group, value, total)
    return total


def unpacked(value, group, last):
    return turned(value, 7 - group if last else -group)


def send_kernel(links, time_out, depth_out, plane_out):
    for face, out in ((0, time_out), (1, depth_out)):
        for slot, direction in enumerate(OTHERS[face]):
            for part in range(2):
                for row in range(2):
                    for col in range(3):
                        source = face_comp(direction, part, row, col)
                        target = face_comp(slot, part, row, col) * 4
                        if face == 0:
                            out[target : target + 4] = links[source, 0:DEPTHS]
                        else:
                            out[target : target + 4] = links[source, pl.ds(0, TIMES, stride=DEPTHS)]
    for part in range(2):
        for row in range(2):
            for col in range(3):
                target = ((part * 2 + row) * 3 + col) * 8
                plane_out[target : target + 8] = packed(
                    [
                        links[face_comp(direction, part, row, col), 8 * half : 8 * half + 8]
                        for half in range(2)
                        for direction in OTHERS[2]
                    ],
                    False,
                )


def matrix(ref, base, rows):
    return [
        [(ref[base + row * 3 + col, rows], ref[base + 9 + row * 3 + col, rows]) for col in range(3)]
        for row in range(3)
    ]


def face_matrix(ref, slot, size):
    rows = [
        [
            tuple(
                ref[face_comp(slot, part, row, col) * size : (face_comp(slot, part, row, col) + 1) * size]
                for part in range(2)
            )
            for col in range(3)
        ]
        for row in range(2)
    ]
    rows.append(third_row(rows[0], rows[1]))
    return rows


def shift_links(links, time_in, depth_in, plane_in, shifted):
    column = lax.broadcasted_iota(jnp.int32, (8, LANES), 1) % NX
    right_edge = column == NX - 1
    last_plane = lane_group((8, LANES)) == LANES // NX - 1
    for face in range(2):
        received = time_in if face == 0 else depth_in
        for slot, direction in enumerate(OTHERS[face]):
            halo = face_matrix(received, slot, 4)
            for part in range(2):
                for row in range(3):
                    for col in range(3):
                        c = comp(direction, part, row, col)
                        if face == 0:
                            shifted[0, c, 0 : ROWS - 4] = links[c, 4:ROWS]
                            shifted[0, c, ROWS - 4 : ROWS] = halo[row][col][part]
                        else:
                            shifted[1, c, 0 : ROWS - 1] = links[c, 1:ROWS]
                            shifted[1, c, pl.ds(3, TIMES, stride=DEPTHS)] = halo[row][col][part]
    halo = face_matrix(plane_in, 0, 8)
    for part in range(2):
        for row in range(3):
            for col in range(3):
                for slot, direction in enumerate(OTHERS[2]):
                    c = comp(direction, part, row, col)
                    for half in range(2):
                        rows = slice(8 * half, 8 * half + 8)
                        outer = unpacked(halo[row][col][part], 3 * half + slot, True)
                        shifted[2, c, rows] = jnp.where(last_plane, outer, turned(links[c, rows], 7))
    for direction in range(3):
        for offset in range(18):
            c = direction * 18 + offset
            for half in range(2):
                rows = slice(8 * half, 8 * half + 8)
                value = links[c, rows]
                shifted[3, c, rows] = jnp.where(
                    right_edge, pltpu.roll(value, NX - 1, 1), pltpu.roll(value, LANES - 1, 1)
                )


def interior_kernel(links, time_in, depth_in, plane_in, force, shifted, moved):
    shift_links(links, time_in, depth_in, plane_in, shifted)
    for face in range(2):
        for c in range(24):
            moved[face, c, 0:8] = jnp.zeros((8, LANES), jnp.float32)

    def step(half, carry):
        start = pl.multiple_of(half * 8, 8)
        rows = pl.ds(start, 8)
        column = lax.broadcasted_iota(jnp.int32, (8, LANES), 1)
        left_edge = column % NX == 0
        first_plane = column < NX
        fresh = [True] * 4

        def add(direction, values, sign):
            for i in range(8):
                c = direction * 8 + i
                if fresh[direction]:
                    force[c, rows] = values[i] if sign > 0 else -values[i]
                elif sign > 0:
                    force[c, rows] = force[c, rows] + values[i]
                else:
                    force[c, rows] = force[c, rows] - values[i]
            fresh[direction] = False

        def carry_over(direction, step_direction, values, sign):
            if step_direction < 2:
                slot = OTHERS[step_direction].index(direction)
                lower = pl.ds(pl.multiple_of(start + 8, 8), 8)
                for i in range(8):
                    moved[step_direction, slot * 8 + i, lower] = values[i] if sign > 0 else -values[i]
                return
            if step_direction == 2:
                values = [jnp.where(first_plane, 0.0, turned(v, 1)) for v in values]
            else:
                values = [
                    jnp.where(left_edge, pltpu.roll(v, LANES - NX + 1, 1), pltpu.roll(v, 1, 1))
                    for v in values
                ]
            add(direction, values, sign)

        for mu, nu in PAIRS:
            link_mu = matrix(links, mu * 18, rows)
            link_nu = matrix(links, nu * 18, rows)
            values = plaquette(
                link_mu,
                matrix(shifted.at[mu], nu * 18, rows),
                link_nu,
                matrix(shifted.at[nu], mu * 18, rows),
            )
            add(mu, values, 1)
            add(nu, values, -1)
            carry_over(mu, nu, rotated(values, link_nu), -1)
            carry_over(nu, mu, rotated(values, link_mu), 1)
        return carry

    lax.fori_loop(0, 2, step, 0)

    inner = row_index((8, LANES)) % DEPTHS != 0
    for direction in range(4):
        for i in range(8):
            c = direction * 8 + i
            for half in range(2):
                rows = slice(8 * half, 8 * half + 8)
                total = force[c, rows]
                if direction != 0:
                    slot = OTHERS[0].index(direction) * 8 + i
                    total = total + moved[0, slot, 8 * half + 4 : 8 * half + 12]
                if direction != 1:
                    slot = OTHERS[1].index(direction) * 8 + i
                    total = total + jnp.where(inner, moved[1, slot, 8 * half + 7 : 8 * half + 15], 0.0)
                force[c, rows] = total


def cells():
    return [(part, row, col) for part in range(2) for row in range(2) for col in range(3)]


def top(ref, face, c):
    return ref[c, 12:16] if face == 0 else ref[c, pl.ds(3, TIMES, stride=DEPTHS)]


def x_ahead(value):
    right_edge = lax.broadcasted_iota(jnp.int32, value.shape, 1) % NX == NX - 1
    return jnp.where(right_edge, pltpu.roll(value, NX - 1, 1), pltpu.roll(value, LANES - 1, 1))


def prepare_kernel(pairs, links, left, ahead, base):
    for direction in range(4):
        for half in range(2):
            rows = slice(8 * half, 8 * half + 8)
            whole = [
                [
                    tuple(pairs[face_comp(direction, part, row, col), rows] for part in range(2))
                    for col in range(3)
                ]
                for row in range(2)
            ]
            whole.append(third_row(whole[0], whole[1]))
            for part in range(2):
                for row in range(3):
                    for col in range(3):
                        links[comp(direction, part, row, col), rows] = whole[row][col][part]
    for part in range(2):
        for row in range(3):
            for col in range(3):
                at = part * 9 + row * 3 + col
                base[0, at, 0:4] = top(links, 0, comp(0, part, row, col))
                base[0, at, 4:8] = top(links, 1, comp(1, part, row, col))
                c = comp(2, part, row, col)
                base[1, at] = packed([links[c, 8 * (q // 3) : 8 * (q // 3) + 8] for q in range(6)], True)
    for part, row, col in cells():
        at = face_comp(0, part, row, col)
        whole = part * 9 + row * 3 + col
        for unit in range(3):
            for face in range(2):
                source = comp(OTHERS[face][unit], part, row, col)
                left[unit, at, 4 * face : 4 * face + 4] = top(links, face, source)
        left[3, at] = packed(
            [
                links[comp(direction, part, row, col), 8 * half : 8 * half + 8]
                for half in range(2)
                for direction in OTHERS[2]
            ],
            True,
        )
        ahead[0, at] = jnp.zeros((8, LANES), jnp.float32)
        ahead[0, at, 0:3] = links[comp(0, part, row, col), 13:16]
        ahead[0, at, 4:7] = links[comp(1, part, row, col), pl.ds(7, 3, stride=DEPTHS)]
        ahead[1, at] = turned(base[0, whole], 7)
        ahead[2, at] = x_ahead(base[0, whole])
        c = comp(2, part, row, col)
        upper = links[c, 8:16]
        along_x = x_ahead(base[1, whole])
        group = lane_group((8, LANES))
        for q, value in (
            (0, links[c, 4:12]),
            (1, links[c, 1:9]),
            (3, pltpu.roll(upper, 4, 0)),
            (4, pltpu.roll(upper, 7, 0)),
        ):
            along_x = jnp.where(group == q, turned(value, q + 1), along_x)
        ahead[3, at] = along_x


def wide(ref, row):
    return jnp.broadcast_to(ref[row : row + 1], (8, LANES))


def faces_kernel(left, ahead, base, time_in, depth_in, plane_in, time_out, depth_out):
    boundary((0, 1, 2), left, ahead, base, time_in, depth_in, plane_in, time_out, depth_out, None)


def plane_kernel(left, ahead, base, time_in, depth_in, plane_in, plane_out):
    boundary((3,), left, ahead, base, time_in, depth_in, plane_in, None, None, plane_out)


def boundary(units, left, ahead, base, time_in, depth_in, plane_in, time_out, depth_out, plane_out):
    row_at = row_index((8, LANES))
    group = lane_group((8, LANES))

    def behind(unit, part, row, col):
        if unit == 3:
            at = face_comp(0, part, row, col) * 8
            return plane_in[at : at + 8]
        at = face_comp(unit, part, row, col) * 4
        return jnp.concatenate([time_in[at : at + 4], depth_in[at : at + 4]], axis=0)

    def beside(unit, part, row, col):
        at = face_comp(0, part, row, col)
        own = ahead[unit, at]
        if unit == 0:
            own = jnp.where(row_at == 3, wide(depth_in, at * 4 + 3), own)
            return jnp.where(row_at == 7, wide(time_in, at * 4 + 3), own)
        if unit == 1:
            time_part = turned(pltpu.roll(plane_in[at * 8 : at * 8 + 8], 4, 0), 4)
            depth_part = jnp.where(row_at % 2 == 1, wide(plane_in, at * 8 + 7), wide(plane_in, at * 8 + 3))
            depth_part = jnp.where(row_at < 6, turned(depth_part, 6), turned(depth_part, 3))
            return jnp.where(group == 7, jnp.where(row_at < 4, time_part, depth_part), own)
        if unit == 2:
            return own
        source = face_comp(1, part, row, col) * 4
        later = turned(time_in[source - 4 : source + 4], 4)
        own = jnp.where((group == 3) & (row_at >= 4), later, own)
        for half in range(2):
            first, second = wide(depth_in, source + 2 * half), wide(depth_in, source + 2 * half + 1)
            q = 3 * half + 1
            deeper = turned(jnp.where(row_at < 4, first, second), q + 1)
            own = jnp.where((group == q) & (row_at % 4 == 3), deeper, own)
        return own

    def complete(fetch):
        rows = [[(fetch(0, row, col), fetch(1, row, col)) for col in range(3)] for row in range(2)]
        rows.append(third_row(rows[0], rows[1]))
        return rows

    for unit in units:
        own_base = [
            [tuple(base[unit // 3, part * 9 + row * 3 + col] for part in range(2)) for col in range(3)]
            for row in range(3)
        ]
        own_left = [
            [tuple(left[unit, face_comp(0, part, row, col)] for part in range(2)) for col in range(3)]
            for row in range(2)
        ]
        values = plaquette(
            own_left,
            complete(lambda part, row, col: beside(unit, part, row, col)),
            own_base,
            complete(lambda part, row, col: behind(unit, part, row, col)),
        )
        for i, value in enumerate(rotated(values, own_base)):
            if unit == 3:
                plane_out[8 * i : 8 * i + 8] = value
            else:
                at = (unit * 8 + i) * 4
                time_out[at : at + 4] = value[0:4]
                depth_out[at : at + 4] = value[4:8]


def final_kernel(force, time_in, depth_in, plane_in, out):
    first_plane = lax.broadcasted_iota(jnp.int32, (8, LANES), 1) < NX
    row_at = row_index((8, LANES))
    half_coeff = 0.5 * COEFF
    upper = ((0, 1), (0, 2), (1, 2))

    def total(direction, i, half):
        value = force[direction * 8 + i, 8 * half : 8 * half + 8]
        if direction != 2:
            group = 3 * half + OTHERS[2].index(direction)
            outer = unpacked(plane_in[8 * i : 8 * i + 8], group, False)
            value = value - jnp.where(first_plane, outer, 0.0)
        if direction != 0 and half == 0:
            at = (OTHERS[0].index(direction) * 8 + i) * 4
            later = time_in[at : at + 4]
            value = value - jnp.concatenate([later, jnp.zeros_like(later)], axis=0)
        if direction != 1:
            at = (OTHERS[1].index(direction) * 8 + i) * 4 + 2 * half
            value = value - jnp.where(row_at == 0, wide(depth_in, at), 0.0)
            value = value - jnp.where(row_at == 4, wide(depth_in, at + 1), 0.0)
        return value * half_coeff

    for direction in range(4):
        for half in range(2):
            rows = slice(8 * half, 8 * half + 8)
            for n, (row, col) in enumerate(upper):
                re = total(direction, 2 * n, half)
                im = total(direction, 2 * n + 1, half)
                out[comp(direction, 0, row, col), rows] = re
                out[comp(direction, 0, col, row), rows] = -re
                out[comp(direction, 1, row, col), rows] = im
                out[comp(direction, 1, col, row), rows] = im
            d0 = total(direction, 6, half)
            d1 = total(direction, 7, half)
            zero = jnp.zeros_like(d0)
            for k, value in enumerate((d0, d1, -(d0 + d1))):
                out[comp(direction, 1, k, k), rows] = value
                out[comp(direction, 0, k, k), rows] = zero


def shape(*dims):
    return pltpu.VMEM(dims, jnp.float32)


def move(value, axis, forward):
    count = lax.axis_size(axis)
    step = 1 if forward else count - 1
    moved = lax.ppermute(value, axis, [(i, (i + step) % count) for i in range(count)])
    return pltpu.with_memory_space_constraint(moved, pltpu.VMEM)


def gauge_force(links):
    pairs = pltpu.with_memory_space_constraint(links[:, :, 0:2].reshape(48, ROWS, LANES), pltpu.VMEM)
    faces = pl.pallas_call(
        send_kernel, out_shape=(shape(144, LANES), shape(144, LANES), shape(96, LANES)), name="send"
    )(pairs)
    depth = move(faces[1], "gz", False)
    time = move(faces[0], "ta", False)
    plane = move(faces[2], "gx", False)
    flat, *local = pl.pallas_call(
        prepare_kernel,
        out_shape=(
            shape(72, ROWS, LANES),
            shape(4, 12, 8, LANES),
            shape(4, 12, 8, LANES),
            shape(2, 18, 8, LANES),
        ),
        name="prepare",
    )(pairs)
    flat, *local = [pltpu.with_memory_space_constraint(value, pltpu.VMEM) for value in (flat, *local)]
    sent = pl.pallas_call(faces_kernel, out_shape=(shape(96, LANES), shape(96, LANES)), name="faces")(
        *local, time, depth, plane
    )
    sent_plane = pl.pallas_call(plane_kernel, out_shape=shape(64, LANES), name="plane")(
        *local, time, depth, plane
    )
    force = pl.pallas_call(
        interior_kernel,
        out_shape=shape(32, ROWS, LANES),
        scratch_shapes=[
            pltpu.VMEM((4, 72, ROWS, LANES), jnp.float32),
            pltpu.VMEM((2, 24, 24, LANES), jnp.float32),
        ],
        name="interior",
    )(flat, time, depth, plane)
    depth = move(sent[1], "gz", True)
    time = move(sent[0], "ta", True)
    plane = move(sent_plane, "gx", True)
    out = pl.pallas_call(
        final_kernel,
        out_shape=jax.ShapeDtypeStruct((72, ROWS, LANES), jnp.float32),
        name="final",
    )(pltpu.with_memory_space_constraint(force, pltpu.VMEM), time, depth, plane)
    return out.reshape(links.shape)


def solution(mesh):
    spec = P(None, None, None, None, "ta", "gz", "gx")
    return jax.shard_map(gauge_force, mesh=mesh, in_specs=(spec,), out_specs=spec, check_vma=False)
```

```python
import jax
import jax.numpy as jnp
from jax import lax
from jax.experimental import pallas as pl
from jax.experimental.pallas import tpu as pltpu
from jax.sharding import PartitionSpec as P


NX = 16
COEFF = -1.9

ROWS = 16
LANES = 128
TIMES = 4
DEPTHS = 4
PAIRS = ((0, 1), (0, 2), (0, 3), (1, 2), (1, 3), (2, 3))
OTHERS = tuple(tuple(d for d in range(4) if d != face) for face in range(3))


def comp(direction, part, row, col):
    return ((direction * 2 + part) * 3 + row) * 3 + col


def face_comp(slot, part, row, col):
    return ((slot * 2 + part) * 2 + row) * 3 + col


def accumulate(terms):
    total = None
    for sign, left, right in terms:
        product = left * right
        if total is None:
            total = product if sign > 0 else -product
        else:
            total = total + product if sign > 0 else total - product
    return total


def product_rows(left, right):
    out = []
    for row in left:
        cols = []
        for j in range(3):
            re = accumulate(
                [(1, row[k][0], right[k][j][0]) for k in range(3)]
                + [(-1, row[k][1], right[k][j][1]) for k in range(3)]
            )
            im = accumulate(
                [(1, row[k][0], right[k][j][1]) for k in range(3)]
                + [(1, row[k][1], right[k][j][0]) for k in range(3)]
            )
            cols.append((re, im))
        out.append(cols)
    return out


def product_rows_dagger(left, right):
    out = []
    for row in left:
        cols = []
        for j in range(3):
            re = accumulate(
                [(1, row[k][0], right[j][k][0]) for k in range(3)]
                + [(1, row[k][1], right[j][k][1]) for k in range(3)]
            )
            im = accumulate(
                [(1, row[k][1], right[j][k][0]) for k in range(3)]
                + [(-1, row[k][0], right[j][k][1]) for k in range(3)]
            )
            cols.append((re, im))
        out.append(cols)
    return out


def cross_real(row0, row1, j):
    a, b = (j + 1) % 3, (j + 2) % 3
    return accumulate(
        [
            (1, row0[a][0], row1[b][0]),
            (-1, row0[a][1], row1[b][1]),
            (-1, row0[b][0], row1[a][0]),
            (1, row0[b][1], row1[a][1]),
        ]
    )


def cross_imag(row0, row1, j):
    a, b = (j + 1) % 3, (j + 2) % 3
    return accumulate(
        [
            (1, row0[b][0], row1[a][1]),
            (1, row0[b][1], row1[a][0]),
            (-1, row0[a][0], row1[b][1]),
            (-1, row0[a][1], row1[b][0]),
        ]
    )


def third_row(row0, row1):
    return [(cross_real(row0, row1, j), cross_imag(row0, row1, j)) for j in range(3)]


def plaquette(left, left_ahead, right, right_ahead):
    first = left if left_ahead is None else product_rows(left[:2], left_ahead)
    second = product_rows(right[:2], right_ahead)
    second.append(third_row(second[0], second[1]))
    loop = product_rows_dagger(first, second)
    row0, row1 = loop
    re20 = cross_real(row0, row1, 0)
    im20 = cross_imag(row0, row1, 0)
    re21 = cross_real(row0, row1, 1)
    im21 = cross_imag(row0, row1, 1)
    im22 = cross_imag(row0, row1, 2)
    third = (row0[0][1] + row1[1][1] + im22) * (1.0 / 3.0)
    d0 = row0[0][1] - third
    d1 = row1[1][1] - third
    return [
        row0[1][0] - row1[0][0],
        row0[1][1] + row1[0][1],
        row0[2][0] - re20,
        row0[2][1] + im20,
        row1[2][0] - re21,
        row1[2][1] + im21,
        d0 + d0,
        d1 + d1,
    ]


def rotated(force, link):
    r01, i01, r02, i02, r12, i12, d0, d1 = force
    d2 = -(d0 + d1)
    diag = (d0, d1, d2)
    upper = {(0, 1): (r01, i01), (0, 2): (r02, i02), (1, 2): (r12, i12)}
    columns = []
    for j in range(3):
        entries = []
        for k in range(3):
            re_terms = [(-1, diag[k], link[k][j][1])]
            im_terms = [(1, diag[k], link[k][j][0])]
            for l in range(3):
                if l == k:
                    continue
                if l > k:
                    re, im = upper[(k, l)]
                    sign = 1
                else:
                    re, im = upper[(l, k)]
                    sign = -1
                re_terms = [(sign, re, link[l][j][0])] + re_terms + [(-1, im, link[l][j][1])]
                im_terms = [(1, im, link[l][j][0])] + im_terms + [(sign, re, link[l][j][1])]
            re_terms.sort(key=lambda term: -term[0])
            entries.append((accumulate(re_terms), accumulate(im_terms)))
        columns.append(entries)

    def real(i, j):
        return accumulate(
            [(1, link[k][i][0], columns[j][k][0]) for k in range(3)]
            + [(1, link[k][i][1], columns[j][k][1]) for k in range(3)]
        )

    def imag(i, j):
        return accumulate(
            [(1, link[k][i][0], columns[j][k][1]) for k in range(3)]
            + [(-1, link[k][i][1], columns[j][k][0]) for k in range(3)]
        )

    return [real(0, 1), imag(0, 1), real(0, 2), imag(0, 2), real(1, 2), imag(1, 2), imag(0, 0), imag(1, 1)]


def lane_group(shape):
    return lax.broadcasted_iota(jnp.int32, shape, 1) // NX


def row_index(shape):
    return lax.broadcasted_iota(jnp.int32, shape, 0)


def turned(value, groups):
    return pltpu.roll(value, groups % 8 * NX, 1) if groups % 8 else value


def packed(values, last):
    total = None
    for group, value in enumerate(values):
        value = turned(value, group + 1 if last else group)
        total = value if total is None else jnp.where(lane_group(value.shape) == group, value, total)
    return total


def unpacked(value, group, last):
    return turned(value, 7 - group if last else -group)


def send_kernel(links, time_out, depth_out, plane_out):
    for face, out in ((0, time_out), (1, depth_out)):
        for slot, direction in enumerate(OTHERS[face]):
            for part in range(2):
                for row in range(2):
                    for col in range(3):
                        source = face_comp(direction, part, row, col)
                        target = face_comp(slot, part, row, col) * 4
                        if face == 0:
                            out[target : target + 4] = links[source, 0:DEPTHS]
                        else:
                            out[target : target + 4] = links[source, pl.ds(0, TIMES, stride=DEPTHS)]
    for part in range(2):
        for row in range(2):
            for col in range(3):
                target = ((part * 2 + row) * 3 + col) * 8
                plane_out[target : target + 8] = packed(
                    [
                        links[face_comp(direction, part, row, col), 8 * half : 8 * half + 8]
                        for half in range(2)
                        for direction in OTHERS[2]
                    ],
                    False,
                )


def matrix(ref, base, rows):
    return [
        [(ref[base + row * 3 + col, rows], ref[base + 9 + row * 3 + col, rows]) for col in range(3)]
        for row in range(3)
    ]


def face_matrix(ref, slot, size):
    rows = [
        [
            tuple(
                ref[face_comp(slot, part, row, col) * size : (face_comp(slot, part, row, col) + 1) * size]
                for part in range(2)
            )
            for col in range(3)
        ]
        for row in range(2)
    ]
    rows.append(third_row(rows[0], rows[1]))
    return rows


def shift_links(links, time_in, depth_in, plane_in, shifted):
    column = lax.broadcasted_iota(jnp.int32, (8, LANES), 1) % NX
    right_edge = column == NX - 1
    last_plane = lane_group((8, LANES)) == LANES // NX - 1
    for face in range(2):
        received = time_in if face == 0 else depth_in
        for slot, direction in enumerate(OTHERS[face]):
            halo = face_matrix(received, slot, 4)
            for part in range(2):
                for row in range(3):
                    for col in range(3):
                        c = comp(direction, part, row, col)
                        if face == 0:
                            shifted[0, c, 0 : ROWS - 4] = links[c, 4:ROWS]
                            shifted[0, c, ROWS - 4 : ROWS] = halo[row][col][part]
                        else:
                            shifted[1, c, 0 : ROWS - 1] = links[c, 1:ROWS]
                            shifted[1, c, pl.ds(3, TIMES, stride=DEPTHS)] = halo[row][col][part]
    halo = face_matrix(plane_in, 0, 8)
    for part in range(2):
        for row in range(3):
            for col in range(3):
                for slot, direction in enumerate(OTHERS[2]):
                    c = comp(direction, part, row, col)
                    for half in range(2):
                        rows = slice(8 * half, 8 * half + 8)
                        outer = unpacked(halo[row][col][part], 3 * half + slot, True)
                        shifted[2, c, rows] = jnp.where(last_plane, outer, turned(links[c, rows], 7))
    for direction in range(3):
        for offset in range(18):
            c = direction * 18 + offset
            for half in range(2):
                rows = slice(8 * half, 8 * half + 8)
                value = links[c, rows]
                shifted[3, c, rows] = jnp.where(
                    right_edge, pltpu.roll(value, NX - 1, 1), pltpu.roll(value, LANES - 1, 1)
                )


def interior_kernel(links, time_in, depth_in, plane_in, force, shifted, moved):
    shift_links(links, time_in, depth_in, plane_in, shifted)
    for face in range(2):
        for c in range(24):
            moved[face, c, 0:8] = jnp.zeros((8, LANES), jnp.float32)

    def step(half, carry):
        start = pl.multiple_of(half * 8, 8)
        rows = pl.ds(start, 8)
        column = lax.broadcasted_iota(jnp.int32, (8, LANES), 1)
        left_edge = column % NX == 0
        first_plane = column < NX
        fresh = [True] * 4

        def add(direction, values, sign):
            for i in range(8):
                c = direction * 8 + i
                if fresh[direction]:
                    force[c, rows] = values[i] if sign > 0 else -values[i]
                elif sign > 0:
                    force[c, rows] = force[c, rows] + values[i]
                else:
                    force[c, rows] = force[c, rows] - values[i]
            fresh[direction] = False

        def carry_over(direction, step_direction, values, sign):
            if step_direction < 2:
                slot = OTHERS[step_direction].index(direction)
                lower = pl.ds(pl.multiple_of(start + 8, 8), 8)
                for i in range(8):
                    moved[step_direction, slot * 8 + i, lower] = values[i] if sign > 0 else -values[i]
                return
            if step_direction == 2:
                values = [jnp.where(first_plane, 0.0, turned(v, 1)) for v in values]
            else:
                values = [
                    jnp.where(left_edge, pltpu.roll(v, LANES - NX + 1, 1), pltpu.roll(v, 1, 1))
                    for v in values
                ]
            add(direction, values, sign)

        for mu, nu in PAIRS:
            link_mu = matrix(links, mu * 18, rows)
            link_nu = matrix(links, nu * 18, rows)
            values = plaquette(
                link_mu,
                matrix(shifted.at[mu], nu * 18, rows),
                link_nu,
                matrix(shifted.at[nu], mu * 18, rows),
            )
            add(mu, values, 1)
            add(nu, values, -1)
            carry_over(mu, nu, rotated(values, link_nu), -1)
            carry_over(nu, mu, rotated(values, link_mu), 1)
        return carry

    lax.fori_loop(0, 2, step, 0)

    inner = row_index((8, LANES)) % DEPTHS != 0
    for direction in range(4):
        for i in range(8):
            c = direction * 8 + i
            for half in range(2):
                rows = slice(8 * half, 8 * half + 8)
                total = force[c, rows]
                if direction != 0:
                    slot = OTHERS[0].index(direction) * 8 + i
                    total = total + moved[0, slot, 8 * half + 4 : 8 * half + 12]
                if direction != 1:
                    slot = OTHERS[1].index(direction) * 8 + i
                    total = total + jnp.where(inner, moved[1, slot, 8 * half + 7 : 8 * half + 15], 0.0)
                force[c, rows] = total


def cells():
    return [(part, row, col) for part in range(2) for row in range(2) for col in range(3)]


def top(ref, face, c):
    return ref[c, 12:16] if face == 0 else ref[c, pl.ds(3, TIMES, stride=DEPTHS)]


def x_ahead(value):
    right_edge = lax.broadcasted_iota(jnp.int32, value.shape, 1) % NX == NX - 1
    return jnp.where(right_edge, pltpu.roll(value, NX - 1, 1), pltpu.roll(value, LANES - 1, 1))


def prepare_kernel(pairs, links, left, ahead, base):
    for direction in range(4):
        for half in range(2):
            rows = slice(8 * half, 8 * half + 8)
            whole = [
                [
                    tuple(pairs[face_comp(direction, part, row, col), rows] for part in range(2))
                    for col in range(3)
                ]
                for row in range(2)
            ]
            whole.append(third_row(whole[0], whole[1]))
            for part in range(2):
                for row in range(3):
                    for col in range(3):
                        links[comp(direction, part, row, col), rows] = whole[row][col][part]
    for part in range(2):
        for row in range(3):
            for col in range(3):
                at = part * 9 + row * 3 + col
                base[0, at, 0:4] = top(links, 0, comp(0, part, row, col))
                base[0, at, 4:8] = top(links, 1, comp(1, part, row, col))
                c = comp(2, part, row, col)
                base[1, at] = packed([links[c, 8 * (q // 3) : 8 * (q // 3) + 8] for q in range(6)], True)
    for part, row, col in cells():
        at = face_comp(0, part, row, col)
        whole = part * 9 + row * 3 + col
        for unit in range(3):
            for face in range(2):
                source = comp(OTHERS[face][unit], part, row, col)
                left[unit, at, 4 * face : 4 * face + 4] = top(links, face, source)
        left[3, at] = packed(
            [
                links[comp(direction, part, row, col), 8 * half : 8 * half + 8]
                for half in range(2)
                for direction in OTHERS[2]
            ],
            True,
        )
        ahead[0, at] = jnp.zeros((8, LANES), jnp.float32)
        ahead[0, at, 0:3] = links[comp(0, part, row, col), 13:16]
        ahead[0, at, 4:7] = links[comp(1, part, row, col), pl.ds(7, 3, stride=DEPTHS)]
        ahead[1, at] = turned(base[0, whole], 7)
        c = comp(2, part, row, col)
        upper = links[c, 8:16]
        along_x = x_ahead(base[1, whole])
        group = lane_group((8, LANES))
        for q, value in (
            (0, links[c, 4:12]),
            (1, links[c, 1:9]),
            (3, pltpu.roll(upper, 4, 0)),
            (4, pltpu.roll(upper, 7, 0)),
        ):
            along_x = jnp.where(group == q, turned(value, q + 1), along_x)
        ahead[3, at] = along_x


    along = [
        [tuple(x_ahead(base[0, part * 9 + row * 3 + col]) for part in range(2)) for col in range(3)]
        for row in range(3)
    ]
    own = [
        [tuple(left[2, face_comp(0, part, row, col)] for part in range(2)) for col in range(3)]
        for row in range(2)
    ]
    for row, values in enumerate(product_rows(own, along)):
        for col in range(3):
            for part in range(2):
                ahead[2, face_comp(0, part, row, col)] = values[col][part]


def wide(ref, row):
    return jnp.broadcast_to(ref[row : row + 1], (8, LANES))


def faces_kernel(left, ahead, base, time_in, depth_in, plane_in, time_out, depth_out):
    boundary((0, 1, 2), left, ahead, base, time_in, depth_in, plane_in, time_out, depth_out, None)


def plane_kernel(left, ahead, base, time_in, depth_in, plane_in, plane_out):
    boundary((3,), left, ahead, base, time_in, depth_in, plane_in, None, None, plane_out)


def boundary(units, left, ahead, base, time_in, depth_in, plane_in, time_out, depth_out, plane_out):
    row_at = row_index((8, LANES))
    group = lane_group((8, LANES))

    def behind(unit, part, row, col):
        if unit == 3:
            at = face_comp(0, part, row, col) * 8
            return plane_in[at : at + 8]
        at = face_comp(unit, part, row, col) * 4
        return jnp.concatenate([time_in[at : at + 4], depth_in[at : at + 4]], axis=0)

    def beside(unit, part, row, col):
        at = face_comp(0, part, row, col)
        own = ahead[unit, at]
        if unit == 0:
            own = jnp.where(row_at == 3, wide(depth_in, at * 4 + 3), own)
            return jnp.where(row_at == 7, wide(time_in, at * 4 + 3), own)
        if unit == 1:
            time_part = turned(pltpu.roll(plane_in[at * 8 : at * 8 + 8], 4, 0), 4)
            depth_part = jnp.where(row_at % 2 == 1, wide(plane_in, at * 8 + 7), wide(plane_in, at * 8 + 3))
            depth_part = jnp.where(row_at < 6, turned(depth_part, 6), turned(depth_part, 3))
            return jnp.where(group == 7, jnp.where(row_at < 4, time_part, depth_part), own)
        source = face_comp(1, part, row, col) * 4
        later = turned(time_in[source - 4 : source + 4], 4)
        own = jnp.where((group == 3) & (row_at >= 4), later, own)
        for half in range(2):
            first, second = wide(depth_in, source + 2 * half), wide(depth_in, source + 2 * half + 1)
            q = 3 * half + 1
            deeper = turned(jnp.where(row_at < 4, first, second), q + 1)
            own = jnp.where((group == q) & (row_at % 4 == 3), deeper, own)
        return own

    def complete(fetch):
        rows = [[(fetch(0, row, col), fetch(1, row, col)) for col in range(3)] for row in range(2)]
        rows.append(third_row(rows[0], rows[1]))
        return rows

    for unit in units:
        own_base = [
            [tuple(base[unit // 3, part * 9 + row * 3 + col] for part in range(2)) for col in range(3)]
            for row in range(3)
        ]
        own_left = [
            [
                tuple((ahead if unit == 2 else left)[unit, face_comp(0, part, row, col)] for part in range(2))
                for col in range(3)
            ]
            for row in range(2)
        ]
        values = plaquette(
            own_left,
            None if unit == 2 else complete(lambda part, row, col: beside(unit, part, row, col)),
            own_base,
            complete(lambda part, row, col: behind(unit, part, row, col)),
        )
        for i, value in enumerate(rotated(values, own_base)):
            if unit == 3:
                plane_out[8 * i : 8 * i + 8] = value
            else:
                at = (unit * 8 + i) * 4
                time_out[at : at + 4] = value[0:4]
                depth_out[at : at + 4] = value[4:8]


def final_kernel(force, time_in, depth_in, plane_in, out):
    first_plane = lax.broadcasted_iota(jnp.int32, (8, LANES), 1) < NX
    row_at = row_index((8, LANES))
    half_coeff = 0.5 * COEFF
    upper = ((0, 1), (0, 2), (1, 2))

    def total(direction, i, half):
        value = force[direction * 8 + i, 8 * half : 8 * half + 8]
        if direction != 2:
            group = 3 * half + OTHERS[2].index(direction)
            outer = unpacked(plane_in[8 * i : 8 * i + 8], group, False)
            value = value - jnp.where(first_plane, outer, 0.0)
        if direction != 0 and half == 0:
            at = (OTHERS[0].index(direction) * 8 + i) * 4
            later = time_in[at : at + 4]
            value = value - jnp.concatenate([later, jnp.zeros_like(later)], axis=0)
        if direction != 1:
            at = (OTHERS[1].index(direction) * 8 + i) * 4 + 2 * half
            value = value - jnp.where(row_at == 0, wide(depth_in, at), 0.0)
            value = value - jnp.where(row_at == 4, wide(depth_in, at + 1), 0.0)
        return value * half_coeff

    for direction in range(4):
        for half in range(2):
            rows = slice(8 * half, 8 * half + 8)
            for n, (row, col) in enumerate(upper):
                re = total(direction, 2 * n, half)
                im = total(direction, 2 * n + 1, half)
                out[comp(direction, 0, row, col), rows] = re
                out[comp(direction, 0, col, row), rows] = -re
                out[comp(direction, 1, row, col), rows] = im
                out[comp(direction, 1, col, row), rows] = im
            d0 = total(direction, 6, half)
            d1 = total(direction, 7, half)
            zero = jnp.zeros_like(d0)
            for k, value in enumerate((d0, d1, -(d0 + d1))):
                out[comp(direction, 1, k, k), rows] = value
                out[comp(direction, 0, k, k), rows] = zero


def shape(*dims):
    return pltpu.VMEM(dims, jnp.float32)


def move(value, axis, forward):
    count = lax.axis_size(axis)
    step = 1 if forward else count - 1
    moved = lax.ppermute(value, axis, [(i, (i + step) % count) for i in range(count)])
    return pltpu.with_memory_space_constraint(moved, pltpu.VMEM)


def gauge_force(links):
    pairs = pltpu.with_memory_space_constraint(links[:, :, 0:2].reshape(48, ROWS, LANES), pltpu.VMEM)
    faces = pl.pallas_call(
        send_kernel, out_shape=(shape(144, LANES), shape(144, LANES), shape(96, LANES)), name="send"
    )(pairs)
    depth = move(faces[1], "gz", False)
    time = move(faces[0], "ta", False)
    plane = move(faces[2], "gx", False)
    flat, *local = pl.pallas_call(
        prepare_kernel,
        out_shape=(
            shape(72, ROWS, LANES),
            shape(4, 12, 8, LANES),
            shape(4, 12, 8, LANES),
            shape(2, 18, 8, LANES),
        ),
        name="prepare",
    )(pairs)
    flat, *local = [pltpu.with_memory_space_constraint(value, pltpu.VMEM) for value in (flat, *local)]
    sent = pl.pallas_call(faces_kernel, out_shape=(shape(96, LANES), shape(96, LANES)), name="faces")(
        *local, time, depth, plane
    )
    sent_plane = pl.pallas_call(plane_kernel, out_shape=shape(64, LANES), name="plane")(
        *local, time, depth, plane
    )
    force = pl.pallas_call(
        interior_kernel,
        out_shape=shape(32, ROWS, LANES),
        scratch_shapes=[
            pltpu.VMEM((4, 72, ROWS, LANES), jnp.float32),
            pltpu.VMEM((2, 24, 24, LANES), jnp.float32),
        ],
        name="interior",
    )(flat, time, depth, plane)
    depth = move(sent[1], "gz", True)
    time = move(sent[0], "ta", True)
    plane = move(sent_plane, "gx", True)
    out = pl.pallas_call(
        final_kernel,
        out_shape=jax.ShapeDtypeStruct((72, ROWS, LANES), jnp.float32),
        name="final",
    )(pltpu.with_memory_space_constraint(force, pltpu.VMEM), time, depth, plane)
    return out.reshape(links.shape)


def solution(mesh):
    spec = P(None, None, None, None, "ta", "gz", "gx")
    return jax.shard_map(gauge_force, mesh=mesh, in_specs=(spec,), out_specs=spec, check_vma=False)
```
